32 devices in a mesh: gx: 4 (over x, core), gy: 2 (over y), gz: 4 (over z).
Axes of the slice: x: 2, y: 2, z: 4, core: 2. Of those that a mesh axis runs over, the one named last changes fastest.
Arguments:
- fields: float32 [32, 32, 16, 512], P(None, 'gx', 'gy', 'gz'), may hold values from -8 to 8
- strength: float32 [32], replicated, may hold values from 0.3 to 1
Outputs:
- filtered: float32 [32, 32, 16, 512], P(None, 'gx', 'gy', 'gz')
The draws below stay inside these ranges and needn't reach their ends.
All inputs are finite; a program needn't handle non-finite values.
Results may differ from the reference program's by a relative error of at most 0.00002.
Values sent between devices are 32-bit elements; how exact they have to be, the bound alone decides.
A program may use at most 64 MiB of HBM per device.

```python
import math
import jax
import jax.numpy as jnp
from jax import lax

SPECIES = 32
NX = 32
NY = 16
NZ = 512


def steps_of(own_key, extent, shards, smallest, top_value):
    def one(axis_at, shards_of):
        draws = jax.random.uniform(jax.random.fold_in(jax.random.fold_in(own_key, 6), axis_at), (shards_of,), jnp.float32, smallest / len(shards), top_value / len(shards))
        return jnp.repeat(jnp.exp(draws), extent[axis_at] // shards_of).reshape((-1,) + (1,) * (len(extent) - axis_at - 1))

    gain = one(*shards[0])
    for cut in shards[1:]:
        gain = gain * one(*cut)
    return gain


def scatter_about(own_key, shape, scale, reach, split=(), kind=jnp.bfloat16):
    values = jax.random.normal(own_key, shape, jnp.float32) * scale
    if len(split) > 0:
        values = steps_of(own_key, shape, split, -0.22, 0.18) * values
    return jnp.clip(values, min=-reach, max=reach).astype(kind)


def setup_inputs(seed: int = 0) -> dict:
    key_of = jax.random.split(jax.random.key(seed), 3)
    fields = scatter_about(key_of[0], (SPECIES, NX, NY, NZ), 1.0, 8.0, ((1, 4), (2, 2), (3, 4)), jnp.float32)
    strength = jnp.clip(jnp.exp(jax.random.uniform(key_of[1], (SPECIES,), jnp.float32, math.log(0.3), math.log(1.0))), 0.3, 1.0)
    return {"fields": fields, "strength": strength}


filter_weights = [1.0, -10.0, 45.0, -120.0, 210.0, -252.0, 210.0, -120.0, 45.0, -10.0, 1.0]


def tenth_difference(field, axis):
    total = jnp.zeros(field.shape, jnp.float32)
    for index in range(11):
        total = total + filter_weights[index] * jnp.roll(field, 5 - index, axis)
    return total


def filter_species(packed):
    field, scale = packed
    summed = tenth_difference(field, 0) + tenth_difference(field, 1) + tenth_difference(field, 2)
    return field + (scale / 1024.0) * summed


def reference(fields, strength):
    return lax.map(filter_species, (fields, strength))
```

```python
import functools
import jax
import jax.numpy as jnp
from jax import lax
from jax.experimental import pallas as pl
from jax.experimental.pallas import tpu as pltpu
from jax.sharding import PartitionSpec as P

MESH = pl.DeviceIdType.MESH
REACH = 5
SLOT = 8
WEIGHTS = [-252.0, 210.0, -120.0, 45.0, -10.0, 1.0]
CUTS = (2, 8, 8, 6, 3, 2, 2, 1)
EARLY = 4


def weight_of(offset):
    return WEIGHTS[abs(offset)] if abs(offset) <= REACH else 0.0


def row_weights(rows, lanes, roll, bases):
    row = lax.broadcasted_iota(jnp.int32, (rows, lanes), 0)
    out = jnp.zeros((rows, lanes), jnp.float32)
    for i in range(rows):
        value = sum(weight_of((i + roll) % rows + base - i) for base in bases)
        if value:
            out = jnp.where(row == i, value, out)
    return out


def rolled_rows(block, roll):
    rows = block.shape[1]
    return block if roll == 0 else pltpu.roll(block, rows - roll, 1)


def rows_sum(block, weights):
    total = None
    for roll, weight in enumerate(weights):
        term = weight[None] * rolled_rows(block, roll)
        total = term if total is None else total + term
    return total


def kernel(nx, ny, nz, cuts, early, fields, strength_in, out, strength, u, acc, xl, xr, ys, packed, landed,
           in_sem, x_send, x_recv, y_send, y_recv, z_send, z_recv, answers, turn):
    species, cx, cy, cz = u.shape
    groups = cz // SLOT
    rows_packed = packed.shape[1]
    px, py, pz = lax.axis_index("gx"), lax.axis_index("gy"), lax.axis_index("gz")
    x_left, x_right = lax.rem(px + nx - 1, nx), lax.rem(px + 1, nx)
    y_left, y_right = lax.rem(py + ny - 1, ny), lax.rem(py + 1, ny)
    z_left, z_right = lax.rem(pz + nz - 1, nz), lax.rem(pz + 1, nz)
    y_peers = [y_right] if ny == 2 else [y_right, y_left]

    barrier = pltpu.get_barrier_semaphore()
    to_left, to_right = (px, py, z_left), (px, py, z_right)
    left_x, right_x = (x_left, py, pz), (x_right, py, pz)
    first_x, last_x, first_z, last_z = px == 0, px == nx - 1, pz == 0, pz == nz - 1

    def tell(semaphore, peer):
        pl.semaphore_signal(semaphore, inc=1, device_id=peer, device_id_type=MESH)

    for peer in y_peers:
        tell(barrier, (px, peer, pz))
    pl.when(px < nx - 1)(lambda: tell(barrier, right_x))
    pl.when(first_x)(lambda: tell(barrier, left_x))
    pl.when(pz < nz - 1)(lambda: tell(barrier, to_right))

    spans = []
    begin = 0
    for size in cuts:
        spans.append((begin, size))
        begin += size
    loads = []
    for k, (begin, size) in enumerate(spans):
        part = pl.ds(begin, size)
        loads.append(pltpu.make_async_copy(fields.at[part], u.at[part], in_sem.at[k]))
    gains = pltpu.make_async_copy(strength_in, strength, in_sem.at[len(cuts)])
    for load in loads:
        load.start()
    gains.start()

    held = early < len(cuts)
    odd = lax.rem(px, 2) == 1
    y_copies, x_copies = [], []
    for k, (begin, size) in enumerate(spans):
        part = pl.ds(begin, size)
        row = []
        for side, peer in enumerate(y_peers):
            row.append(pltpu.make_async_remote_copy(
                src_ref=u.at[part], dst_ref=ys.at[side, part],
                send_sem=y_send.at[side, k], recv_sem=y_recv.at[side, k],
                device_id=(px, peer, pz), device_id_type=MESH))
        y_copies.append(row)
        x_copies.append([
            pltpu.make_async_remote_copy(
                src_ref=u.at[part, pl.ds(cx - REACH, REACH)], dst_ref=xl.at[part],
                send_sem=x_send.at[0, k], recv_sem=x_recv.at[0, k],
                device_id=(x_right, py, pz), device_id_type=MESH),
            pltpu.make_async_remote_copy(
                src_ref=u.at[part, pl.ds(0, REACH)], dst_ref=xr.at[part],
                send_sem=x_send.at[1, k], recv_sem=x_recv.at[1, k],
                device_id=(x_left, py, pz), device_id_type=MESH),
        ])

    def start_y(rows):
        for row in rows:
            for copy in row:
                copy.start()

    def sent_y(rows):
        for row in rows:
            for copy in row:
                copy.wait_send()

    greeters = sum(c.astype(jnp.int32) for c in (px > 0, last_x, pz > 0))
    pl.semaphore_wait(barrier, len(y_peers) + greeters)
    for load, row in zip(loads[:early], y_copies[:early]):
        load.wait()
        start_y([row])
    for load in loads[early:]:
        load.wait()
    if held:
        pl.when(jnp.logical_not(odd))(lambda: start_y(y_copies[early:]))
    pl.when(px > 0)(lambda: tell(answers.at[0], left_x))
    pl.when(last_x)(lambda: tell(answers.at[1], right_x))
    pl.when(last_z)(lambda: tell(answers.at[2], to_left))
    gains.wait()
    pl.when(px < nx - 1)(lambda: pl.semaphore_wait(answers.at[0], 1))
    pl.when(first_x)(lambda: pl.semaphore_wait(answers.at[1], 1))
    for row in x_copies:
        for copy in row:
            copy.start()

    lane = lax.broadcasted_iota(jnp.int32, (cx, cy, cz), 2)
    slot = lane // SLOT
    for p in range(rows_packed):
        first = p * groups
        here = min(groups, species - first)

        def pack(g, carry):
            head, tail = carry
            v = u[first + g]
            mine = slot == g
            head = jnp.where(mine, pltpu.roll(v, g * SLOT, 2), head)
            tail = jnp.where(mine, pltpu.roll(v, lax.rem((g + 1) * SLOT, cz), 2), tail)
            return head, tail

        zero = jnp.zeros((cx, cy, cz), jnp.float32)
        head, tail = lax.fori_loop(0, here, pack, (zero, zero))
        packed[0, p] = head
        packed[1, p] = tail

    pl.when(pz < nz - 1)(lambda: pl.semaphore_wait(answers.at[2], 1))
    pl.when(jnp.logical_and(pz > 0, pz < nz - 1))(lambda: tell(answers.at[2], to_left))
    pl.when(first_z)(lambda: tell(answers.at[3], to_left))
    pl.when(last_z)(lambda: pl.semaphore_wait(answers.at[3], 1))
    z_copies = [
        pltpu.make_async_remote_copy(
            src_ref=packed.at[side], dst_ref=landed.at[side],
            send_sem=z_send.at[side], recv_sem=z_recv.at[side],
            device_id=(px, py, peer), device_id_type=MESH)
        for side, peer in enumerate((z_left, z_right))
    ]
    for copy in z_copies:
        copy.start()

    own = [row_weights(cy, cz, r, (0,)) for r in range(cy)]
    if ny == 2:
        remote = [[row_weights(cy, cz, r, (cy, -cy)) for r in range(cy)]]
    else:
        remote = [[row_weights(cy, cz, r, (base,)) for r in range(cy)] for base in (-cy, cy)]

    for copy in z_copies:
        copy.wait()

    def along_z(s, _):
        v = u[s]
        p, g = s // groups, lax.rem(s, groups)
        after = pltpu.roll(landed[0, p], lax.rem(cz - g * SLOT, cz), 2)
        before = pltpu.roll(landed[1, p], cz - (g + 1) * SLOT, 2)
        total = (2.0 * WEIGHTS[0]) * v
        for d in range(1, REACH + 1):
            up = pltpu.roll(jnp.where(lane < d, after, v), cz - d, 2)
            down = pltpu.roll(jnp.where(lane >= cz - d, before, v), d, 2)
            total = total + WEIGHTS[d] * (up + down)
        acc[s] = total + rows_sum(v, own)
        return 0

    lax.fori_loop(0, species, along_z, 0)

    def along_x(s, _):
        cells = [xl[s, i] for i in range(REACH)] + [u[s, i] for i in range(cx)]
        cells += [xr[s, i] for i in range(REACH)]
        for i in range(cx):
            total = acc[s, i]
            for d in range(1, REACH + 1):
                total = total + WEIGHTS[d] * (cells[REACH + i - d] + cells[REACH + i + d])
            acc[s, i] = total
        return 0

    def along_y(s, _):
        total = acc[s]
        for side, weights in enumerate(remote):
            total = total + rows_sum(ys[side, s], weights)
        out[s] = u[s] + (strength[s] * (1.0 / 1024.0)) * total
        return 0

    def take_turn():
        def pass_on():
            sent_y(y_copies[:early + 1])
            tell(turn, right_x)

        def go_on():
            pl.semaphore_wait(turn, 1)
            start_y(y_copies[early:])

        pl.when(odd)(go_on)
        pl.when(jnp.logical_not(odd))(pass_on)

    for k, (begin, size) in enumerate(spans):
        if k == early:
            take_turn()
        for copy in x_copies[k]:
            copy.wait_recv()
        lax.fori_loop(begin, begin + size, along_x, 0)
        for copy in y_copies[k]:
            copy.wait_recv()
        lax.fori_loop(begin, begin + size, along_y, 0)
    for row in x_copies:
        for copy in row:
            copy.wait_send()
    if held:
        pl.when(odd)(lambda: sent_y(y_copies[:early + 1]))
        sent_y(y_copies[early + 1:])
    else:
        sent_y(y_copies)


def local(nx, ny, nz, fields, strength):
    species, cx, cy, cz = fields.shape
    cuts = CUTS if sum(CUTS) == species else (1,) * species
    pieces = len(cuts)
    early = EARLY if sum(CUTS) == species and nx % 2 == 0 else pieces
    sides = 1 if ny == 2 else 2
    groups = cz // SLOT
    rows_packed = -(-species // groups)
    block = (species, cx, cy, cz)
    dma = pltpu.SemaphoreType.DMA
    return pl.pallas_call(
        functools.partial(kernel, nx, ny, nz, cuts, early),
        out_shape=pltpu.VMEM(block, jnp.float32),
        in_specs=[pl.BlockSpec(memory_space=pltpu.HBM), pl.BlockSpec(memory_space=pl.ANY)],
        out_specs=pl.BlockSpec(memory_space=pltpu.VMEM),
        scratch_shapes=[
            pltpu.SMEM((species,), jnp.float32),
            pltpu.VMEM(block, jnp.float32),
            pltpu.VMEM(block, jnp.float32),
            pltpu.VMEM((species, REACH, cy, cz), jnp.float32),
            pltpu.VMEM((species, REACH, cy, cz), jnp.float32),
            pltpu.VMEM((sides,) + block, jnp.float32),
            pltpu.VMEM((2, rows_packed, cx, cy, cz), jnp.float32),
            pltpu.VMEM((2, rows_packed, cx, cy, cz), jnp.float32),
            dma((pieces + 1,)),
            dma((2, pieces)),
            dma((2, pieces)),
            dma((sides, pieces)),
            dma((sides, pieces)),
            dma((2,)),
            dma((2,)),
            pltpu.SemaphoreType.REGULAR((4,)),
            pltpu.SemaphoreType.REGULAR,
        ],
        compiler_params=pltpu.CompilerParams(collective_id=0, has_side_effects=True, vmem_limit_bytes=56 * 1024 * 1024),
        name="filter_pass",
    )(fields, strength)


def solution(mesh):
    sizes = mesh.shape
    return jax.shard_map(
        functools.partial(local, sizes["gx"], sizes["gy"], sizes["gz"]),
        mesh=mesh,
        in_specs=(P(None, "gx", "gy", "gz"), P()),
        out_specs=P(None, "gx", "gy", "gz"),
        check_vma=False,
    )
```

```python
import functools
import jax
import jax.numpy as jnp
from jax import lax
from jax.experimental import pallas as pl
from jax.experimental.pallas import tpu as pltpu
from jax.sharding import PartitionSpec as P

MESH = pl.DeviceIdType.MESH
REACH = 5
SLOT = 8
WEIGHTS = [-252.0, 210.0, -120.0, 45.0, -10.0, 1.0]
CUTS = (2, 8, 8, 6, 3, 2, 2, 1)
EARLY = 4
X_PIECES = 2
AT_ONCE = (8, 4, 8)


def each(begin, count, at_once, body, carry=0):
    step = at_once if count % at_once == 0 else 1

    def steps(k, carry):
        for i in range(step):
            carry = body(begin + k * step + i, carry)
        return carry

    return lax.fori_loop(0, count // step, steps, carry)


def weight_of(offset):
    return WEIGHTS[abs(offset)] if abs(offset) <= REACH else 0.0


def row_weights(rows, lanes, roll, bases):
    row = lax.broadcasted_iota(jnp.int32, (rows, lanes), 0)
    out = jnp.zeros((rows, lanes), jnp.float32)
    for i in range(rows):
        value = sum(weight_of((i + roll) % rows + base - i) for base in bases)
        if value:
            out = jnp.where(row == i, value, out)
    return out


def lane_weights(lanes, bases, centre):
    source = lax.broadcasted_iota(jnp.int32, (lanes, lanes), 0)
    offset = source - lax.broadcasted_iota(jnp.int32, (lanes, lanes), 1)
    out = jnp.zeros((lanes, lanes), jnp.float32)
    for base in bases:
        for d in range(-REACH, REACH + 1):
            out = jnp.where(offset + base == d, centre if d == 0 else weight_of(d), out)
    return out.astype(jnp.bfloat16)


def along_lanes(rows, weights):
    total = None
    for part in range(3):
        piece = rows.astype(jnp.bfloat16)
        rows = rows - piece.astype(jnp.float32)
        term = jnp.dot(piece, weights, preferred_element_type=jnp.float32)
        total = term if total is None else total + term
    return total


def rolled_rows(block, roll):
    rows = block.shape[1]
    return block if roll == 0 else pltpu.roll(block, rows - roll, 1)


def rows_sum(block, weights):
    total = None
    for roll, weight in enumerate(weights):
        term = weight[None] * rolled_rows(block, roll)
        total = term if total is None else total + term
    return total


def kernel(nx, ny, nz, cuts, early, x_size, fields, strength_in, out, strength, u, acc, xl, xr, ys, packed, landed,
           in_sem, x_send, x_recv, y_send, y_recv, z_send, z_recv, answers, turn):
    species, cx, cy, cz = u.shape
    groups = cz // SLOT
    rows_packed = packed.shape[1]
    px, py, pz = lax.axis_index("gx"), lax.axis_index("gy"), lax.axis_index("gz")
    x_left, x_right = lax.rem(px + nx - 1, nx), lax.rem(px + 1, nx)
    y_left, y_right = lax.rem(py + ny - 1, ny), lax.rem(py + 1, ny)
    z_left, z_right = lax.rem(pz + nz - 1, nz), lax.rem(pz + 1, nz)
    y_peers = [y_right] if ny == 2 else [y_right, y_left]

    barrier = pltpu.get_barrier_semaphore()
    to_left, to_right = (px, py, z_left), (px, py, z_right)
    left_x, right_x = (x_left, py, pz), (x_right, py, pz)
    first_x, last_x, first_z, last_z = px == 0, px == nx - 1, pz == 0, pz == nz - 1

    def tell(semaphore, peer):
        pl.semaphore_signal(semaphore, inc=1, device_id=peer, device_id_type=MESH)

    for peer in y_peers:
        tell(barrier, (px, peer, pz))
    pl.when(px < nx - 1)(lambda: tell(barrier, right_x))
    pl.when(first_x)(lambda: tell(barrier, left_x))
    pl.when(pz < nz - 1)(lambda: tell(barrier, to_right))

    spans = []
    begin = 0
    for size in cuts:
        spans.append((begin, size))
        begin += size
    loads = []
    for k, (begin, size) in enumerate(spans):
        part = pl.ds(begin, size)
        loads.append(pltpu.make_async_copy(fields.at[part], u.at[part], in_sem.at[k]))
    gains = pltpu.make_async_copy(strength_in, strength, in_sem.at[len(cuts)])
    for load in loads:
        load.start()
    gains.start()

    held = early < len(cuts)
    odd = lax.rem(px, 2) == 1
    y_copies, x_copies = [], []
    for k, (begin, size) in enumerate(spans):
        part = pl.ds(begin, size)
        row = []
        for side, peer in enumerate(y_peers):
            row.append(pltpu.make_async_remote_copy(
                src_ref=u.at[part], dst_ref=ys.at[side, part],
                send_sem=y_send.at[side, k], recv_sem=y_recv.at[side, k],
                device_id=(px, peer, pz), device_id_type=MESH))
        y_copies.append(row)
    x_spans = [(at, x_size) for at in range(0, species, x_size)]
    for k, (begin, size) in enumerate(x_spans):
        part = pl.ds(begin, size)
        x_copies.append([
            pltpu.make_async_remote_copy(
                src_ref=u.at[part, pl.ds(cx - REACH, REACH)], dst_ref=xl.at[part],
                send_sem=x_send.at[0, k], recv_sem=x_recv.at[0, k],
                device_id=(x_right, py, pz), device_id_type=MESH),
            pltpu.make_async_remote_copy(
                src_ref=u.at[part, pl.ds(0, REACH)], dst_ref=xr.at[part],
                send_sem=x_send.at[1, k], recv_sem=x_recv.at[1, k],
                device_id=(x_left, py, pz), device_id_type=MESH),
        ])

    def start_y(rows):
        for row in rows:
            for copy in row:
                copy.start()

    def sent_y(rows):
        for row in rows:
            for copy in row:
                copy.wait_send()

    greeters = sum(c.astype(jnp.int32) for c in (px > 0, last_x, pz > 0))
    pl.semaphore_wait(barrier, len(y_peers) + greeters)
    for load, row in zip(loads[:early], y_copies[:early]):
        load.wait()
        start_y([row])
    for load in loads[early:]:
        load.wait()
    if held:
        pl.when(jnp.logical_not(odd))(lambda: start_y(y_copies[early:]))
    pl.when(px > 0)(lambda: tell(answers.at[0], left_x))
    pl.when(last_x)(lambda: tell(answers.at[1], right_x))
    pl.when(pz > 0)(lambda: tell(answers.at[2], to_left))
    pl.when(last_z)(lambda: tell(answers.at[4], to_left))
    gains.wait()
    pl.when(px < nx - 1)(lambda: pl.semaphore_wait(answers.at[0], 1))
    pl.when(first_x)(lambda: pl.semaphore_wait(answers.at[1], 1))
    for row in x_copies:
        for copy in row:
            copy.start()

    lane = lax.broadcasted_iota(jnp.int32, (cx, cy, cz), 2)
    slot = lane // SLOT
    for p in range(rows_packed):
        first = p * groups
        here = min(groups, species - first)

        def pack(g, carry):
            head, tail = carry
            v = u[first + g]
            mine = slot == g
            head = jnp.where(mine, pltpu.roll(v, g * SLOT, 2), head)
            tail = jnp.where(mine, pltpu.roll(v, lax.rem((g + 1) * SLOT, cz), 2), tail)
            return head, tail

        zero = jnp.zeros((cx, cy, cz), jnp.float32)
        head, tail = each(0, here, AT_ONCE[0], pack, (zero, zero))
        packed[0, p] = head
        packed[1, p] = tail

    z_copies = [
        pltpu.make_async_remote_copy(
            src_ref=packed.at[side], dst_ref=landed.at[side],
            send_sem=z_send.at[side], recv_sem=z_recv.at[side],
            device_id=(px, py, peer), device_id_type=MESH)
        for side, peer in enumerate((z_left, z_right))
    ]

    def start_right():
        pl.semaphore_wait(answers.at[2], 1)
        z_copies[1].start()

    def pass_token():
        pl.semaphore_wait(answers.at[4], 1)
        tell(answers.at[4], to_left)

    def close_ring():
        pl.semaphore_wait(answers.at[4], 1)
        tell(answers.at[3], to_left)
        z_copies[0].start()

    def end_ring():
        pl.semaphore_wait(answers.at[3], 1)
        z_copies[1].start()

    pl.when(pz > 0)(z_copies[0].start)
    pl.when(pz < nz - 1)(start_right)
    pl.when(jnp.logical_and(pz > 0, pz < nz - 1))(pass_token)
    pl.when(first_z)(close_ring)

    own = [row_weights(cy, cz, r, (0,)) for r in range(cy)]
    if ny == 2:
        remote = [[row_weights(cy, cz, r, (cy, -cy)) for r in range(cy)]]
    else:
        remote = [[row_weights(cy, cz, r, (base,)) for r in range(cy)] for base in (-cy, cy)]
    inside = lane_weights(cz, (0,), 2.0 * WEIGHTS[0])
    across = lane_weights(cz, (cz, -cz), WEIGHTS[0])

    def along_own(s, _):
        v = u[s]
        total = along_lanes(v.reshape(cx * cy, cz), inside).reshape(cx, cy, cz)
        acc[s] = total + rows_sum(v, own)
        return 0

    each(0, species, AT_ONCE[1], along_own)
    pl.when(last_z)(end_ring)
    for copy in z_copies:
        copy.wait()

    def along_z(s, _):
        p, g = s // groups, lax.rem(s, groups)
        after = pltpu.roll(landed[0, p], lax.rem(cz - g * SLOT, cz), 2)
        before = pltpu.roll(landed[1, p], cz - (g + 1) * SLOT, 2)
        halo = jnp.where(lane < cz // 2, after, before)
        acc[s] = acc[s] + along_lanes(halo.reshape(cx * cy, cz), across).reshape(cx, cy, cz)
        return 0

    each(0, species, AT_ONCE[2], along_z)

    def along_x(s, _):
        cells = [xl[s, i] for i in range(REACH)] + [u[s, i] for i in range(cx)]
        cells += [xr[s, i] for i in range(REACH)]
        for i in range(cx):
            total = acc[s, i]
            for d in range(1, REACH + 1):
                total = total + WEIGHTS[d] * (cells[REACH + i - d] + cells[REACH + i + d])
            acc[s, i] = total
        return 0

    def along_y(s, _):
        total = acc[s]
        for side, weights in enumerate(remote):
            total = total + rows_sum(ys[side, s], weights)
        out[s] = u[s] + (strength[s] * (1.0 / 1024.0)) * total
        return 0

    def take_turn():
        def pass_on():
            sent_y(y_copies[:early + 1])
            tell(turn, right_x)

        def go_on():
            pl.semaphore_wait(turn, 1)
            start_y(y_copies[early:])

        pl.when(odd)(go_on)
        pl.when(jnp.logical_not(odd))(pass_on)

    for k, (begin, size) in enumerate(x_spans):
        for copy in x_copies[k]:
            copy.wait_recv()
        lax.fori_loop(begin, begin + size, along_x, 0)
    for k, (begin, size) in enumerate(spans):
        if k == early:
            take_turn()
        for copy in y_copies[k]:
            copy.wait_recv()
        lax.fori_loop(begin, begin + size, along_y, 0)
    for row in x_copies:
        for copy in row:
            copy.wait_send()
    if held:
        pl.when(odd)(lambda: sent_y(y_copies[:early + 1]))
        sent_y(y_copies[early + 1:])
    else:
        sent_y(y_copies)


def local(nx, ny, nz, fields, strength):
    species, cx, cy, cz = fields.shape
    cuts = CUTS if sum(CUTS) == species else (1,) * species
    pieces = len(cuts)
    early = EARLY if sum(CUTS) == species and nx % 2 == 0 else pieces
    x_size = species // X_PIECES if species % X_PIECES == 0 else 1
    sides = 1 if ny == 2 else 2
    groups = cz // SLOT
    rows_packed = -(-species // groups)
    block = (species, cx, cy, cz)
    dma = pltpu.SemaphoreType.DMA
    return pl.pallas_call(
        functools.partial(kernel, nx, ny, nz, cuts, early, x_size),
        out_shape=pltpu.VMEM(block, jnp.float32),
        in_specs=[pl.BlockSpec(memory_space=pltpu.HBM), pl.BlockSpec(memory_space=pl.ANY)],
        out_specs=pl.BlockSpec(memory_space=pltpu.VMEM),
        scratch_shapes=[
            pltpu.SMEM((species,), jnp.float32),
            pltpu.VMEM(block, jnp.float32),
            pltpu.VMEM(block, jnp.float32),
            pltpu.VMEM((species, REACH, cy, cz), jnp.float32),
            pltpu.VMEM((species, REACH, cy, cz), jnp.float32),
            pltpu.VMEM((sides,) + block, jnp.float32),
            pltpu.VMEM((2, rows_packed, cx, cy, cz), jnp.float32),
            pltpu.VMEM((2, rows_packed, cx, cy, cz), jnp.float32),
            dma((pieces + 1,)),
            dma((2, species // x_size)),
            dma((2, species // x_size)),
            dma((sides, pieces)),
            dma((sides, pieces)),
            dma((2,)),
            dma((2,)),
            pltpu.SemaphoreType.REGULAR((5,)),
            pltpu.SemaphoreType.REGULAR,
        ],
        compiler_params=pltpu.CompilerParams(collective_id=0, has_side_effects=True, vmem_limit_bytes=56 * 1024 * 1024),
        name="filter_pass",
    )(fields, strength)


def solution(mesh):
    sizes = mesh.shape
    return jax.shard_map(
        functools.partial(local, sizes["gx"], sizes["gy"], sizes["gz"]),
        mesh=mesh,
        in_specs=(P(None, "gx", "gy", "gz"), P()),
        out_specs=P(None, "gx", "gy", "gz"),
        check_vma=False,
    )
```

```python
import functools
import jax
import jax.numpy as jnp
from jax import lax
from jax.experimental import pallas as pl
from jax.experimental.pallas import tpu as pltpu
from jax.sharding import PartitionSpec as P

MESH = pl.DeviceIdType.MESH
REACH = 5
SLOT = 8
WEIGHTS = [-252.0, 210.0, -120.0, 45.0, -10.0, 1.0]
CUTS = (1, 23, 3, 2, 2, 1)
EARLY = 2
AT_ONCE = (8, 4, 8)


def each(begin, count, at_once, body, carry=0):
    step = at_once if count % at_once == 0 else 1

    def steps(k, carry):
        for i in range(step):
            carry = body(begin + k * step + i, carry)
        return carry

    return lax.fori_loop(0, count // step, steps, carry)


def weight_of(offset):
    return WEIGHTS[abs(offset)] if abs(offset) <= REACH else 0.0


def row_weights(rows, lanes, roll, bases):
    row = lax.broadcasted_iota(jnp.int32, (rows, lanes), 0)
    out = jnp.zeros((rows, lanes), jnp.float32)
    for i in range(rows):
        value = sum(weight_of((i + roll) % rows + base - i) for base in bases)
        if value:
            out = jnp.where(row == i, value, out)
    return out


def lane_weights(lanes, bases, centre):
    source = lax.broadcasted_iota(jnp.int32, (lanes, lanes), 0)
    offset = source - lax.broadcasted_iota(jnp.int32, (lanes, lanes), 1)
    out = jnp.zeros((lanes, lanes), jnp.float32)
    for base in bases:
        for d in range(-REACH, REACH + 1):
            out = jnp.where(offset + base == d, centre if d == 0 else weight_of(d), out)
    return out.astype(jnp.bfloat16)


def along_lanes(rows, weights):
    total = None
    for part in range(3):
        piece = rows.astype(jnp.bfloat16)
        rows = rows - piece.astype(jnp.float32)
        term = jnp.dot(piece, weights, preferred_element_type=jnp.float32)
        total = term if total is None else total + term
    return total


def rolled_rows(block, roll):
    rows = block.shape[1]
    return block if roll == 0 else pltpu.roll(block, rows - roll, 1)


def rows_sum(block, weights):
    total = None
    for roll, weight in enumerate(weights):
        term = weight[None] * rolled_rows(block, roll)
        total = term if total is None else total + term
    return total


def kernel(nx, ny, nz, cuts, early, fields, strength_in, out, strength, u, acc, xs, ys, packed, landed,
           in_sem, x_send, x_recv, y_send, y_recv, z_send, z_recv, answers, turn):
    species, cx, cy, cz = u.shape
    groups = cz // SLOT
    rows_packed = packed.shape[1]
    px, py, pz = lax.axis_index("gx"), lax.axis_index("gy"), lax.axis_index("gz")
    x_left, x_right = lax.rem(px + nx - 1, nx), lax.rem(px + 1, nx)
    y_left, y_right = lax.rem(py + ny - 1, ny), lax.rem(py + 1, ny)
    z_left, z_right = lax.rem(pz + nz - 1, nz), lax.rem(pz + 1, nz)
    y_peers = [y_right] if ny == 2 else [y_right, y_left]

    barrier = pltpu.get_barrier_semaphore()
    to_left, to_right = (px, py, z_left), (px, py, z_right)
    left_x, right_x = (x_left, py, pz), (x_right, py, pz)
    first_x, last_x, first_z, last_z = px == 0, px == nx - 1, pz == 0, pz == nz - 1

    def tell(semaphore, peer):
        pl.semaphore_signal(semaphore, inc=1, device_id=peer, device_id_type=MESH)

    for peer in y_peers:
        tell(barrier, (px, peer, pz))
    pl.when(px < nx - 1)(lambda: tell(barrier, right_x))
    pl.when(first_x)(lambda: tell(barrier, left_x))
    pl.when(pz < nz - 1)(lambda: tell(barrier, to_right))

    spans = []
    begin = 0
    for size in cuts:
        spans.append((begin, size))
        begin += size
    head, rest = pl.ds(0, cuts[0]), pl.ds(cuts[0], species - cuts[0])
    loads = [pltpu.make_async_copy(fields.at[part], u.at[part], in_sem.at[k]) for k, part in enumerate((head, rest))]
    gains = pltpu.make_async_copy(strength_in, strength, in_sem.at[2])
    for load in loads:
        load.start()
    gains.start()

    held = early < len(cuts)
    odd = lax.rem(px, 2) == 1
    mark = sum(cuts[:early + 1])
    y_copies = []
    for k, (begin, size) in enumerate(spans):
        part = pl.ds(begin, size)
        y_copies.append([
            pltpu.make_async_remote_copy(
                src_ref=u.at[part], dst_ref=ys.at[side, part],
                send_sem=y_send.at[side, int(begin >= mark)], recv_sem=y_recv.at[side, k],
                device_id=(px, peer, pz), device_id_type=MESH)
            for side, peer in enumerate(y_peers)])
    x_copies = [
        pltpu.make_async_remote_copy(
            src_ref=u.at[:, pl.ds(begin, REACH)], dst_ref=xs.at[side],
            send_sem=x_send, recv_sem=x_recv,
            device_id=(peer, py, pz), device_id_type=MESH)
        for side, (begin, peer) in enumerate(((cx - REACH, x_right), (0, x_left)))
    ]

    def settle(ref, semaphore):
        pltpu.make_async_copy(ref, ref, semaphore).wait()

    def start_y(rows):
        for row in rows:
            for copy in row:
                copy.start()

    def sent_y(group):
        part = pl.ds(0, mark) if group == 0 else pl.ds(mark, species - mark)
        for side in range(len(y_peers)):
            settle(u.at[part], y_send.at[side, group])

    greeters = sum(c.astype(jnp.int32) for c in (px > 0, last_x, pz > 0))
    pl.semaphore_wait(barrier, len(y_peers) + greeters)
    loads[0].wait()
    start_y(y_copies[:1])
    loads[1].wait()
    start_y(y_copies[1:early])
    if held:
        pl.when(jnp.logical_not(odd))(lambda: start_y(y_copies[early:]))
    pl.when(px > 0)(lambda: tell(answers.at[0], left_x))
    pl.when(last_x)(lambda: tell(answers.at[0], right_x))
    pl.when(pz > 0)(lambda: tell(answers.at[1], to_left))
    pl.when(last_z)(lambda: tell(answers.at[2], to_left))
    gains.wait()
    pl.when(px < nx - 1)(lambda: pl.semaphore_wait(answers.at[0], first_x.astype(jnp.int32) + 1))
    for copy in x_copies:
        copy.start()

    lane = lax.broadcasted_iota(jnp.int32, (cx, cy, cz), 2)
    slot = lane // SLOT
    for p in range(rows_packed):
        first = p * groups
        here = min(groups, species - first)

        def pack(g, carry):
            head, tail = carry
            v = u[first + g]
            mine = slot == g
            head = jnp.where(mine, pltpu.roll(v, g * SLOT, 2), head)
            tail = jnp.where(mine, pltpu.roll(v, lax.rem((g + 1) * SLOT, cz), 2), tail)
            return head, tail

        zero = jnp.zeros((cx, cy, cz), jnp.float32)
        head, tail = each(0, here, AT_ONCE[0], pack, (zero, zero))
        packed[0, p] = head
        packed[1, p] = tail

    z_copies = [
        pltpu.make_async_remote_copy(
            src_ref=packed.at[side], dst_ref=landed.at[side],
            send_sem=z_send, recv_sem=z_recv,
            device_id=(px, py, peer), device_id_type=MESH)
        for side, peer in enumerate((z_left, z_right))
    ]

    def start_right():
        pl.semaphore_wait(answers.at[1], 1)
        z_copies[1].start()

    def pass_token():
        pl.semaphore_wait(answers.at[2], 1)
        tell(answers.at[2], to_left)

    def close_ring():
        pl.semaphore_wait(answers.at[2], 1)
        tell(answers.at[1], to_left)
        z_copies[0].start()

    def end_ring():
        pl.semaphore_wait(answers.at[1], 1)
        z_copies[1].start()

    pl.when(pz < nz - 1)(start_right)
    pl.when(pz > 0)(z_copies[0].start)
    pl.when(jnp.logical_and(pz > 0, pz < nz - 1))(pass_token)
    pl.when(first_z)(close_ring)

    own = [row_weights(cy, cz, r, (0,)) for r in range(cy)]
    if ny == 2:
        remote = [[row_weights(cy, cz, r, (cy, -cy)) for r in range(cy)]]
    else:
        remote = [[row_weights(cy, cz, r, (base,)) for r in range(cy)] for base in (-cy, cy)]
    inside = lane_weights(cz, (0,), 2.0 * WEIGHTS[0])
    across = lane_weights(cz, (cz, -cz), WEIGHTS[0])

    def along_own(s, _):
        v = u[s]
        total = along_lanes(v.reshape(cx * cy, cz), inside).reshape(cx, cy, cz)
        acc[s] = total + rows_sum(v, own)
        return 0

    each(0, species, AT_ONCE[1], along_own)
    pl.when(last_z)(end_ring)
    settle(landed, z_recv)

    def along_z(s, _):
        p, g = s // groups, lax.rem(s, groups)
        after = pltpu.roll(landed[0, p], lax.rem(cz - g * SLOT, cz), 2)
        before = pltpu.roll(landed[1, p], cz - (g + 1) * SLOT, 2)
        halo = jnp.where(lane < cz // 2, after, before)
        acc[s] = acc[s] + along_lanes(halo.reshape(cx * cy, cz), across).reshape(cx, cy, cz)
        return 0

    each(0, species, AT_ONCE[2], along_z)

    def along_x(s, _):
        cells = [xs[0, s, i] for i in range(REACH)] + [u[s, i] for i in range(cx)]
        cells += [xs[1, s, i] for i in range(REACH)]
        for i in range(cx):
            total = acc[s, i]
            for d in range(1, REACH + 1):
                total = total + WEIGHTS[d] * (cells[REACH + i - d] + cells[REACH + i + d])
            acc[s, i] = total
        return 0

    def along_y(s, _):
        total = acc[s]
        for side, weights in enumerate(remote):
            total = total + rows_sum(ys[side, s], weights)
        out[s] = u[s] + (strength[s] * (1.0 / 1024.0)) * total
        return 0

    settle(xs, x_recv)
    lax.fori_loop(0, species, along_x, 0)
    if held:
        def go_on():
            pl.semaphore_wait(turn, 1)
            start_y(y_copies[early:])

        def pass_on():
            sent_y(0)
            tell(turn, right_x)

        pl.when(odd)(go_on)
        pl.when(jnp.logical_not(odd))(pass_on)
    for k, (begin, size) in enumerate(spans):
        for copy in y_copies[k]:
            copy.wait_recv()
        lax.fori_loop(begin, begin + size, along_y, 0)
    settle(xs, x_send)
    settle(packed, z_send)
    if held:
        pl.when(odd)(lambda: sent_y(0))
    else:
        sent_y(0)
    if mark < species:
        sent_y(1)


def local(nx, ny, nz, fields, strength):
    species, cx, cy, cz = fields.shape
    cuts = CUTS if sum(CUTS) == species else (1,) * species
    pieces = len(cuts)
    early = EARLY if sum(CUTS) == species and nx % 2 == 0 else pieces
    sides = 1 if ny == 2 else 2
    groups = cz // SLOT
    rows_packed = -(-species // groups)
    block = (species, cx, cy, cz)
    dma = pltpu.SemaphoreType.DMA
    return pl.pallas_call(
        functools.partial(kernel, nx, ny, nz, cuts, early),
        out_shape=pltpu.VMEM(block, jnp.float32),
        in_specs=[pl.BlockSpec(memory_space=pltpu.HBM), pl.BlockSpec(memory_space=pl.ANY)],
        out_specs=pl.BlockSpec(memory_space=pltpu.VMEM),
        scratch_shapes=[
            pltpu.SMEM((species,), jnp.float32),
            pltpu.VMEM(block, jnp.float32),
            pltpu.VMEM(block, jnp.float32),
            pltpu.VMEM((2, species, REACH, cy, cz), jnp.float32),
            pltpu.VMEM((sides,) + block, jnp.float32),
            pltpu.VMEM((2, rows_packed, cx, cy, cz), jnp.float32),
            pltpu.VMEM((2, rows_packed, cx, cy, cz), jnp.float32),
            dma((3,)),
            dma,
            dma,
            dma((sides, 2)),
            dma((sides, pieces)),
            dma,
            dma,
            pltpu.SemaphoreType.REGULAR((3,)),
            pltpu.SemaphoreType.REGULAR,
        ],
        compiler_params=pltpu.CompilerParams(collective_id=0, has_side_effects=True, vmem_limit_bytes=56 * 1024 * 1024),
        name="filter_pass",
    )(fields, strength)


def solution(mesh):
    sizes = mesh.shape
    return jax.shard_map(
        functools.partial(local, sizes["gx"], sizes["gy"], sizes["gz"]),
        mesh=mesh,
        in_specs=(P(None, "gx", "gy", "gz"), P()),
        out_specs=P(None, "gx", "gy", "gz"),
        check_vma=False,
    )
```

```python
import functools
import jax
import jax.numpy as jnp
from jax import lax
from jax.experimental import pallas as pl
from jax.experimental.pallas import tpu as pltpu
from jax.sharding import PartitionSpec as P

MESH = pl.DeviceIdType.MESH
REACH = 5
SLOT = 8
WEIGHTS = [-252.0, 210.0, -120.0, 45.0, -10.0, 1.0]
CUTS = (24, 3, 2, 2, 1)
EARLY = 1
AT_ONCE = (8, 4, 8)


def each(begin, count, at_once, body, carry=0):
    step = at_once if count % at_once == 0 else 1

    def steps(k, carry):
        for i in range(step):
            carry = body(begin + k * step + i, carry)
        return carry

    return lax.fori_loop(0, count // step, steps, carry)


def weight_of(offset):
    return WEIGHTS[abs(offset)] if abs(offset) <= REACH else 0.0


def row_weights(rows, lanes, roll, bases):
    row = lax.broadcasted_iota(jnp.int32, (rows, lanes), 0)
    out = jnp.zeros((rows, lanes), jnp.float32)
    for i in range(rows):
        value = sum(weight_of((i + roll) % rows + base - i) for base in bases)
        if value:
            out = jnp.where(row == i, value, out)
    return out


def lane_weights(lanes, bases, centre):
    source = lax.broadcasted_iota(jnp.int32, (lanes, lanes), 0)
    offset = source - lax.broadcasted_iota(jnp.int32, (lanes, lanes), 1)
    out = jnp.zeros((lanes, lanes), jnp.float32)
    for base in bases:
        for d in range(-REACH, REACH + 1):
            out = jnp.where(offset + base == d, centre if d == 0 else weight_of(d), out)
    return out.astype(jnp.bfloat16)


def along_lanes(rows, weights):
    total = None
    for part in range(3):
        piece = rows.astype(jnp.bfloat16)
        rows = rows - piece.astype(jnp.float32)
        term = jnp.dot(piece, weights, preferred_element_type=jnp.float32)
        total = term if total is None else total + term
    return total


def rolled_rows(block, roll):
    rows = block.shape[1]
    return block if roll == 0 else pltpu.roll(block, rows - roll, 1)


def rows_sum(block, weights):
    total = None
    for roll, weight in enumerate(weights):
        term = weight[None] * rolled_rows(block, roll)
        total = term if total is None else total + term
    return total


def kernel(nx, ny, nz, cuts, early, fields, strength_in, out, strength, u, acc, xs, ys, packed, landed,
           in_sem, x_send, x_recv, y_send, y_recv, z_send, z_recv, answers, turn):
    species, cx, cy, cz = u.shape
    groups = cz // SLOT
    rows_packed = packed.shape[1]
    px, py, pz = lax.axis_index("gx"), lax.axis_index("gy"), lax.axis_index("gz")
    x_left, x_right = lax.rem(px + nx - 1, nx), lax.rem(px + 1, nx)
    y_left, y_right = lax.rem(py + ny - 1, ny), lax.rem(py + 1, ny)
    z_left, z_right = lax.rem(pz + nz - 1, nz), lax.rem(pz + 1, nz)
    y_peers = [y_right] if ny == 2 else [y_right, y_left]

    barrier = pltpu.get_barrier_semaphore()
    to_left, to_right = (px, py, z_left), (px, py, z_right)
    left_x, right_x = (x_left, py, pz), (x_right, py, pz)
    first_z, last_z = pz == 0, pz == nz - 1

    def tell(semaphore, peer):
        pl.semaphore_signal(semaphore, inc=1, device_id=peer, device_id_type=MESH)

    for peer in y_peers:
        tell(barrier, (px, peer, pz))
    odd = lax.rem(px, 2) == 1
    paired = nx % 2 == 0

    def both_x(semaphore):
        tell(semaphore, left_x)
        tell(semaphore, right_x)

    if paired:
        pl.when(odd)(lambda: both_x(barrier))
    else:
        both_x(barrier)
    pl.when(pz < nz - 1)(lambda: tell(barrier, to_right))

    spans = []
    begin = 0
    for size in cuts:
        spans.append((begin, size))
        begin += size
    load = pltpu.make_async_copy(fields, u, in_sem.at[0])
    gains = pltpu.make_async_copy(strength_in, strength, in_sem.at[1])
    load.start()
    gains.start()

    held = early < len(cuts)
    mark = sum(cuts[:early + 1])
    y_copies = []
    for k, (begin, size) in enumerate(spans):
        part = pl.ds(begin, size)
        y_copies.append([
            pltpu.make_async_remote_copy(
                src_ref=(fields if k < early else u).at[part], dst_ref=ys.at[side, part],
                send_sem=y_send.at[side, int(begin >= mark)], recv_sem=y_recv.at[side, k],
                device_id=(px, peer, pz), device_id_type=MESH)
            for side, peer in enumerate(y_peers)])
    x_copies = [
        pltpu.make_async_remote_copy(
            src_ref=u.at[:, pl.ds(begin, REACH)], dst_ref=xs.at[side],
            send_sem=x_send, recv_sem=x_recv,
            device_id=(peer, py, pz), device_id_type=MESH)
        for side, (begin, peer) in enumerate(((cx - REACH, x_right), (0, x_left)))
    ]

    def settle(ref, semaphore):
        pltpu.make_async_copy(ref, ref, semaphore).wait()

    def start_y(rows):
        for row in rows:
            for copy in row:
                copy.start()

    def sent_y(group):
        part = pl.ds(0, mark) if group == 0 else pl.ds(mark, species - mark)
        for side in range(len(y_peers)):
            settle(u.at[part], y_send.at[side, group])

    greeters = (pz > 0).astype(jnp.int32) + (2 * (1 - lax.rem(px, 2)) if paired else 2)
    pl.semaphore_wait(barrier, len(y_peers) + greeters)
    start_y(y_copies[:early])
    load.wait()
    if held:
        pl.when(jnp.logical_not(odd))(lambda: start_y(y_copies[early:]))
    if paired:
        pl.when(jnp.logical_not(odd))(lambda: both_x(answers.at[0]))
    pl.when(pz > 0)(lambda: tell(answers.at[1], to_left))
    pl.when(last_z)(lambda: tell(answers.at[2], to_left))
    gains.wait()
    if paired:
        pl.when(odd)(lambda: pl.semaphore_wait(answers.at[0], 2))
    for copy in x_copies:
        copy.start()

    lane = lax.broadcasted_iota(jnp.int32, (cx, cy, cz), 2)
    slot = lane // SLOT
    for p in range(rows_packed):
        first = p * groups
        here = min(groups, species - first)

        def pack(g, carry):
            head, tail = carry
            v = u[first + g]
            mine = slot == g
            head = jnp.where(mine, pltpu.roll(v, g * SLOT, 2), head)
            tail = jnp.where(mine, pltpu.roll(v, lax.rem((g + 1) * SLOT, cz), 2), tail)
            return head, tail

        zero = jnp.zeros((cx, cy, cz), jnp.float32)
        head, tail = each(0, here, AT_ONCE[0], pack, (zero, zero))
        packed[0, p] = head
        packed[1, p] = tail

    z_copies = [
        pltpu.make_async_remote_copy(
            src_ref=packed.at[side], dst_ref=landed.at[side],
            send_sem=z_send, recv_sem=z_recv,
            device_id=(px, py, peer), device_id_type=MESH)
        for side, peer in enumerate((z_left, z_right))
    ]

    def start_right():
        pl.semaphore_wait(answers.at[1], 1)
        z_copies[1].start()

    def pass_token():
        pl.semaphore_wait(answers.at[2], 1)
        tell(answers.at[2], to_left)

    def close_ring():
        pl.semaphore_wait(answers.at[2], 1)
        tell(answers.at[1], to_left)
        z_copies[0].start()

    def end_ring():
        pl.semaphore_wait(answers.at[1], 1)
        z_copies[1].start()

    pl.when(pz < nz - 1)(start_right)
    pl.when(pz > 0)(z_copies[0].start)
    pl.when(jnp.logical_and(pz > 0, pz < nz - 1))(pass_token)
    pl.when(first_z)(close_ring)

    own = [row_weights(cy, cz, r, (0,)) for r in range(cy)]
    if ny == 2:
        remote = [[row_weights(cy, cz, r, (cy, -cy)) for r in range(cy)]]
    else:
        remote = [[row_weights(cy, cz, r, (base,)) for r in range(cy)] for base in (-cy, cy)]
    inside = lane_weights(cz, (0,), 2.0 * WEIGHTS[0])
    across = lane_weights(cz, (cz, -cz), WEIGHTS[0])

    def along_own(s, _):
        v = u[s]
        total = along_lanes(v.reshape(cx * cy, cz), inside).reshape(cx, cy, cz)
        acc[s] = total + rows_sum(v, own)
        return 0

    each(0, species, AT_ONCE[1], along_own)
    pl.when(last_z)(end_ring)
    settle(landed, z_recv)

    def along_z(s, _):
        p, g = s // groups, lax.rem(s, groups)
        after = pltpu.roll(landed[0, p], lax.rem(cz - g * SLOT, cz), 2)
        before = pltpu.roll(landed[1, p], cz - (g + 1) * SLOT, 2)
        halo = jnp.where(lane < cz // 2, after, before)
        acc[s] = acc[s] + along_lanes(halo.reshape(cx * cy, cz), across).reshape(cx, cy, cz)
        return 0

    each(0, species, AT_ONCE[2], along_z)

    def along_x(s, _):
        cells = [xs[0, s, i] for i in range(REACH)] + [u[s, i] for i in range(cx)]
        cells += [xs[1, s, i] for i in range(REACH)]
        for i in range(cx):
            total = acc[s, i]
            for d in range(1, REACH + 1):
                total = total + WEIGHTS[d] * (cells[REACH + i - d] + cells[REACH + i + d])
            acc[s, i] = total
        return 0

    def along_y(s, _):
        total = acc[s]
        for side, weights in enumerate(remote):
            total = total + rows_sum(ys[side, s], weights)
        out[s] = u[s] + (strength[s] * (1.0 / 1024.0)) * total
        return 0

    settle(xs, x_recv)
    lax.fori_loop(0, species, along_x, 0)
    if held:
        def go_on():
            pl.semaphore_wait(turn, 1)
            start_y(y_copies[early:])

        def pass_on():
            sent_y(0)
            tell(turn, right_x)

        pl.when(odd)(go_on)
        pl.when(jnp.logical_not(odd))(pass_on)
    for k, (begin, size) in enumerate(spans):
        for copy in y_copies[k]:
            copy.wait_recv()
        lax.fori_loop(begin, begin + size, along_y, 0)
    settle(xs, x_send)
    settle(packed, z_send)
    if held:
        pl.when(odd)(lambda: sent_y(0))
    else:
        sent_y(0)
    if mark < species:
        sent_y(1)


def local(nx, ny, nz, fields, strength):
    species, cx, cy, cz = fields.shape
    cuts = CUTS if sum(CUTS) == species else (1,) * species
    pieces = len(cuts)
    early = EARLY if sum(CUTS) == species and nx % 2 == 0 else pieces
    sides = 1 if ny == 2 else 2
    groups = cz // SLOT
    rows_packed = -(-species // groups)
    block = (species, cx, cy, cz)
    dma = pltpu.SemaphoreType.DMA
    return pl.pallas_call(
        functools.partial(kernel, nx, ny, nz, cuts, early),
        out_shape=pltpu.VMEM(block, jnp.float32),
        in_specs=[pl.BlockSpec(memory_space=pltpu.HBM), pl.BlockSpec(memory_space=pl.ANY)],
        out_specs=pl.BlockSpec(memory_space=pltpu.VMEM),
        scratch_shapes=[
            pltpu.SMEM((species,), jnp.float32),
            pltpu.VMEM(block, jnp.float32),
            pltpu.VMEM(block, jnp.float32),
            pltpu.VMEM((2, species, REACH, cy, cz), jnp.float32),
            pltpu.VMEM((sides,) + block, jnp.float32),
            pltpu.VMEM((2, rows_packed, cx, cy, cz), jnp.float32),
            pltpu.VMEM((2, rows_packed, cx, cy, cz), jnp.float32),
            dma((2,)),
            dma,
            dma,
            dma((sides, 2)),
            dma((sides, pieces)),
            dma,
            dma,
            pltpu.SemaphoreType.REGULAR((3,)),
            pltpu.SemaphoreType.REGULAR,
        ],
        compiler_params=pltpu.CompilerParams(collective_id=0, has_side_effects=True, vmem_limit_bytes=56 * 1024 * 1024),
        name="filter_pass",
    )(fields, strength)


def solution(mesh):
    sizes = mesh.shape
    return jax.shard_map(
        functools.partial(local, sizes["gx"], sizes["gy"], sizes["gz"]),
        mesh=mesh,
        in_specs=(P(None, "gx", "gy", "gz"), P()),
        out_specs=P(None, "gx", "gy", "gz"),
        check_vma=False,
    )
```

```python
import functools
import jax
import jax.numpy as jnp
from jax import lax
from jax.experimental import pallas as pl
from jax.experimental.pallas import tpu as pltpu
from jax.sharding import PartitionSpec as P

MESH = pl.DeviceIdType.MESH
REACH = 5
SLOT = 8
WEIGHTS = [-252.0, 210.0, -120.0, 45.0, -10.0, 1.0]
CUTS = (23, 1, 3, 2, 2, 1)
EARLY = 2
AT_ONCE = (8, 4, 8)


def each(begin, count, at_once, body, carry=0):
    step = at_once if count % at_once == 0 else 1

    def steps(k, carry):
        for i in range(step):
            carry = body(begin + k * step + i, carry)
        return carry

    return lax.fori_loop(0, count // step, steps, carry)


def weight_of(offset):
    return WEIGHTS[abs(offset)] if abs(offset) <= REACH else 0.0


def row_weights(rows, lanes, roll, bases):
    row = lax.broadcasted_iota(jnp.int32, (rows, lanes), 0)
    out = jnp.zeros((rows, lanes), jnp.float32)
    for i in range(rows):
        value = sum(weight_of((i + roll) % rows + base - i) for base in bases)
        if value:
            out = jnp.where(row == i, value, out)
    return out


def lane_weights(lanes, bases, centre):
    source = lax.broadcasted_iota(jnp.int32, (lanes, lanes), 0)
    offset = source - lax.broadcasted_iota(jnp.int32, (lanes, lanes), 1)
    out = jnp.zeros((lanes, lanes), jnp.float32)
    for base in bases:
        for d in range(-REACH, REACH + 1):
            out = jnp.where(offset + base == d, centre if d == 0 else weight_of(d), out)
    return out.astype(jnp.bfloat16)


def along_lanes(rows, weights):
    total = None
    for part in range(3):
        piece = rows.astype(jnp.bfloat16)
        rows = rows - piece.astype(jnp.float32)
        term = jnp.dot(piece, weights, preferred_element_type=jnp.float32)
        total = term if total is None else total + term
    return total


def rolled_rows(block, roll):
    rows = block.shape[1]
    return block if roll == 0 else pltpu.roll(block, rows - roll, 1)


def rows_sum(block, weights):
    total = None
    for roll, weight in enumerate(weights):
        term = weight[None] * rolled_rows(block, roll)
        total = term if total is None else total + term
    return total


def kernel(nx, ny, nz, cuts, early, fields, strength_in, out, strength, u, acc, xs, ys, packed, landed, via,
           in_sem, x_send, x_recv, y_send, y_recv, z_send, z_recv, via_send, via_recv, answers, turn):
    species, cx, cy, cz = u.shape
    groups = cz // SLOT
    rows_packed = packed.shape[1]
    px, py, pz = lax.axis_index("gx"), lax.axis_index("gy"), lax.axis_index("gz")
    x_left, x_right = lax.rem(px + nx - 1, nx), lax.rem(px + 1, nx)
    y_left, y_right = lax.rem(py + ny - 1, ny), lax.rem(py + 1, ny)
    z_left, z_right = lax.rem(pz + nz - 1, nz), lax.rem(pz + 1, nz)
    y_peers = [y_right] if ny == 2 else [y_right, y_left]

    barrier = pltpu.get_barrier_semaphore()
    to_left, to_right = (px, py, z_left), (px, py, z_right)
    left_x, right_x = (x_left, py, pz), (x_right, py, pz)
    first_z, last_z = pz == 0, pz == nz - 1

    def tell(semaphore, peer):
        pl.semaphore_signal(semaphore, inc=1, device_id=peer, device_id_type=MESH)

    for peer in y_peers:
        tell(barrier, (px, peer, pz))
    odd = lax.rem(px, 2) == 1
    paired = nx % 2 == 0

    def both_x(semaphore):
        tell(semaphore, left_x)
        tell(semaphore, right_x)

    if paired:
        pl.when(odd)(lambda: both_x(barrier))
    else:
        both_x(barrier)
    pl.when(pz < nz - 1)(lambda: tell(barrier, to_right))

    spans = []
    begin = 0
    for size in cuts:
        spans.append((begin, size))
        begin += size
    load = pltpu.make_async_copy(fields, u, in_sem.at[0])
    gains = pltpu.make_async_copy(strength_in, strength, in_sem.at[1])
    load.start()
    gains.start()

    held = early < len(cuts)
    mark = sum(cuts[:early + 1])
    y_copies = []
    for k, (begin, size) in enumerate(spans):
        part = pl.ds(begin, size)
        y_copies.append([
            pltpu.make_async_remote_copy(
                src_ref=(fields if k < early else u).at[part], dst_ref=ys.at[side, part],
                send_sem=y_send.at[side, int(begin >= mark)], recv_sem=y_recv.at[side, k],
                device_id=(px, peer, pz), device_id_type=MESH)
            for side, peer in enumerate(y_peers)])
    x_copies = [
        pltpu.make_async_remote_copy(
            src_ref=u.at[:, pl.ds(begin, REACH)], dst_ref=xs.at[side],
            send_sem=x_send, recv_sem=x_recv,
            device_id=(peer, py, pz), device_id_type=MESH)
        for side, (begin, peer) in enumerate(((cx - REACH, x_right), (0, x_left)))
    ]

    relayed = held and ny == 2 and nz > 1
    on_way = jnp.logical_and(px == 1, pz < 2)
    source = jnp.logical_and(on_way, jnp.logical_and(py == 1, pz == 0))
    relay_out = jnp.logical_and(on_way, jnp.logical_and(py == 1, pz == 1))
    relay_back = jnp.logical_and(on_way, jnp.logical_and(py == 0, pz == 1))
    detour = pl.ds(spans[early - 1][0], via.shape[0])
    hop_out = pltpu.make_async_remote_copy(
        src_ref=u.at[detour], dst_ref=via, send_sem=y_send.at[0, 0], recv_sem=via_recv,
        device_id=to_right, device_id_type=MESH)
    hop_over = pltpu.make_async_remote_copy(
        src_ref=via, dst_ref=via, send_sem=via_send, recv_sem=via_recv,
        device_id=(px, y_right, pz), device_id_type=MESH)
    hop_back = pltpu.make_async_remote_copy(
        src_ref=via, dst_ref=ys.at[0, detour], send_sem=via_send, recv_sem=y_recv.at[0, early - 1],
        device_id=to_left, device_id_type=MESH)

    def settle(ref, semaphore):
        pltpu.make_async_copy(ref, ref, semaphore).wait()

    def start_y(rows):
        for row in rows:
            for copy in row:
                copy.start()

    def sent_y(group):
        part = pl.ds(0, mark) if group == 0 else pl.ds(mark, species - mark)
        for side in range(len(y_peers)):
            settle(u.at[part], y_send.at[side, group])

    greeters = (pz > 0).astype(jnp.int32) + (2 * (1 - lax.rem(px, 2)) if paired else 2)
    pl.semaphore_wait(barrier, len(y_peers) + greeters)
    if relayed:
        start_y(y_copies[:early - 1])
        pl.when(jnp.logical_not(source))(lambda: start_y(y_copies[early - 1:early]))
    else:
        start_y(y_copies[:early])
    load.wait()
    if held:
        pl.when(jnp.logical_not(odd))(lambda: start_y(y_copies[early:]))
    if paired:
        pl.when(jnp.logical_not(odd))(lambda: both_x(answers.at[0]))
    pl.when(pz > 0)(lambda: tell(answers.at[1], to_left))
    pl.when(last_z)(lambda: tell(answers.at[2], to_left))
    gains.wait()
    if paired:
        pl.when(odd)(lambda: pl.semaphore_wait(answers.at[0], 2))
    for copy in x_copies:
        copy.start()

    lane = lax.broadcasted_iota(jnp.int32, (cx, cy, cz), 2)
    slot = lane // SLOT
    for p in range(rows_packed):
        first = p * groups
        here = min(groups, species - first)

        def pack(g, carry):
            head, tail = carry
            v = u[first + g]
            mine = slot == g
            head = jnp.where(mine, pltpu.roll(v, g * SLOT, 2), head)
            tail = jnp.where(mine, pltpu.roll(v, lax.rem((g + 1) * SLOT, cz), 2), tail)
            return head, tail

        zero = jnp.zeros((cx, cy, cz), jnp.float32)
        head, tail = each(0, here, AT_ONCE[0], pack, (zero, zero))
        packed[0, p] = head
        packed[1, p] = tail

    z_copies = [
        pltpu.make_async_remote_copy(
            src_ref=packed.at[side], dst_ref=landed.at[side],
            send_sem=z_send, recv_sem=z_recv,
            device_id=(px, py, peer), device_id_type=MESH)
        for side, peer in enumerate((z_left, z_right))
    ]

    def start_right():
        pl.semaphore_wait(answers.at[1], 1)
        z_copies[1].start()

    def pass_token():
        pl.semaphore_wait(answers.at[2], 1)
        tell(answers.at[2], to_left)

    def close_ring():
        pl.semaphore_wait(answers.at[2], 1)
        tell(answers.at[1], to_left)
        z_copies[0].start()

    def end_ring():
        pl.semaphore_wait(answers.at[1], 1)
        z_copies[1].start()

    def forward(hop):
        settle(via, via_recv)
        hop.start()

    pl.when(pz < nz - 1)(start_right)
    if relayed:
        pl.when(source)(hop_out.start)
    pl.when(pz > 0)(z_copies[0].start)
    pl.when(jnp.logical_and(pz > 0, pz < nz - 1))(pass_token)
    pl.when(first_z)(close_ring)

    own = [row_weights(cy, cz, r, (0,)) for r in range(cy)]
    if ny == 2:
        remote = [[row_weights(cy, cz, r, (cy, -cy)) for r in range(cy)]]
    else:
        remote = [[row_weights(cy, cz, r, (base,)) for r in range(cy)] for base in (-cy, cy)]
    inside = lane_weights(cz, (0,), 2.0 * WEIGHTS[0])
    across = lane_weights(cz, (cz, -cz), WEIGHTS[0])

    def along_own(s, _):
        v = u[s]
        total = along_lanes(v.reshape(cx * cy, cz), inside).reshape(cx, cy, cz)
        acc[s] = total + rows_sum(v, own)
        return 0

    each(0, species, AT_ONCE[1], along_own)
    pl.when(last_z)(end_ring)
    settle(landed, z_recv)

    def along_z(s, _):
        p, g = s // groups, lax.rem(s, groups)
        after = pltpu.roll(landed[0, p], lax.rem(cz - g * SLOT, cz), 2)
        before = pltpu.roll(landed[1, p], cz - (g + 1) * SLOT, 2)
        halo = jnp.where(lane < cz // 2, after, before)
        acc[s] = acc[s] + along_lanes(halo.reshape(cx * cy, cz), across).reshape(cx, cy, cz)
        return 0

    each(0, species, AT_ONCE[2], along_z)
    if relayed:
        pl.when(relay_out)(lambda: forward(hop_over))

    def along_x(s, _):
        cells = [xs[0, s, i] for i in range(REACH)] + [u[s, i] for i in range(cx)]
        cells += [xs[1, s, i] for i in range(REACH)]
        for i in range(cx):
            total = acc[s, i]
            for d in range(1, REACH + 1):
                total = total + WEIGHTS[d] * (cells[REACH + i - d] + cells[REACH + i + d])
            acc[s, i] = total
        return 0

    def along_y(s, _):
        total = acc[s]
        for side, weights in enumerate(remote):
            total = total + rows_sum(ys[side, s], weights)
        out[s] = u[s] + (strength[s] * (1.0 / 1024.0)) * total
        return 0

    settle(xs, x_recv)
    lax.fori_loop(0, species, along_x, 0)
    if held:
        def go_on():
            pl.semaphore_wait(turn, 1)
            start_y(y_copies[early:])

        def pass_on():
            sent_y(0)
            tell(turn, right_x)

        pl.when(odd)(go_on)
        pl.when(jnp.logical_not(odd))(pass_on)
    if relayed:
        pl.when(relay_back)(lambda: forward(hop_back))
    for k, (begin, size) in enumerate(spans):
        for copy in y_copies[k]:
            copy.wait_recv()
        lax.fori_loop(begin, begin + size, along_y, 0)
    settle(xs, x_send)
    settle(packed, z_send)
    if relayed:
        pl.when(jnp.logical_or(relay_out, relay_back))(lambda: settle(via, via_send))
    if held:
        pl.when(odd)(lambda: sent_y(0))
    else:
        sent_y(0)
    if mark < species:
        sent_y(1)


def local(nx, ny, nz, fields, strength):
    species, cx, cy, cz = fields.shape
    cuts = CUTS if sum(CUTS) == species else (1,) * species
    pieces = len(cuts)
    early = EARLY if sum(CUTS) == species and nx % 2 == 0 else pieces
    sides = 1 if ny == 2 else 2
    groups = cz // SLOT
    rows_packed = -(-species // groups)
    block = (species, cx, cy, cz)
    dma = pltpu.SemaphoreType.DMA
    return pl.pallas_call(
        functools.partial(kernel, nx, ny, nz, cuts, early),
        out_shape=pltpu.VMEM(block, jnp.float32),
        in_specs=[pl.BlockSpec(memory_space=pltpu.HBM), pl.BlockSpec(memory_space=pl.ANY)],
        out_specs=pl.BlockSpec(memory_space=pltpu.VMEM),
        scratch_shapes=[
            pltpu.SMEM((species,), jnp.float32),
            pltpu.VMEM(block, jnp.float32),
            pltpu.VMEM(block, jnp.float32),
            pltpu.VMEM((2, species, REACH, cy, cz), jnp.float32),
            pltpu.VMEM((sides,) + block, jnp.float32),
            pltpu.VMEM((2, rows_packed, cx, cy, cz), jnp.float32),
            pltpu.VMEM((2, rows_packed, cx, cy, cz), jnp.float32),
            pltpu.VMEM((cuts[early - 1], cx, cy, cz), jnp.float32),
            dma((2,)),
            dma,
            dma,
            dma((sides, 2)),
            dma((sides, pieces)),
            dma,
            dma,
            dma,
            dma,
            pltpu.SemaphoreType.REGULAR((3,)),
            pltpu.SemaphoreType.REGULAR,
        ],
        compiler_params=pltpu.CompilerParams(collective_id=0, has_side_effects=True, vmem_limit_bytes=56 * 1024 * 1024),
        name="filter_pass",
    )(fields, strength)


def solution(mesh):
    sizes = mesh.shape
    return jax.shard_map(
        functools.partial(local, sizes["gx"], sizes["gy"], sizes["gz"]),
        mesh=mesh,
        in_specs=(P(None, "gx", "gy", "gz"), P()),
        out_specs=P(None, "gx", "gy", "gz"),
        check_vma=False,
    )
```

```python
import functools
import jax
import jax.numpy as jnp
from jax import lax
from jax.experimental import pallas as pl
from jax.experimental.pallas import tpu as pltpu
from jax.sharding import PartitionSpec as P

MESH = pl.DeviceIdType.MESH
REACH = 5
SLOT = 8
WEIGHTS = [-252.0, 210.0, -120.0, 45.0, -10.0, 1.0]
CUTS = (19, 5, 7, 1)
EARLY = 2
DETOUR = 1
AT_ONCE = (8, 4, 8)


def each(begin, count, at_once, body, carry=0):
    step = at_once if count % at_once == 0 else 1

    def steps(k, carry):
        for i in range(step):
            carry = body(begin + k * step + i, carry)
        return carry

    return lax.fori_loop(0, count // step, steps, carry)


def weight_of(offset):
    return WEIGHTS[abs(offset)] if abs(offset) <= REACH else 0.0


def row_weights(rows, lanes, roll, bases):
    row = lax.broadcasted_iota(jnp.int32, (rows, lanes), 0)
    out = jnp.zeros((rows, lanes), jnp.float32)
    for i in range(rows):
        value = sum(weight_of((i + roll) % rows + base - i) for base in bases)
        if value:
            out = jnp.where(row == i, value, out)
    return out


def lane_weights(lanes, bases, centre):
    source = lax.broadcasted_iota(jnp.int32, (lanes, lanes), 0)
    offset = source - lax.broadcasted_iota(jnp.int32, (lanes, lanes), 1)
    out = jnp.zeros((lanes, lanes), jnp.float32)
    for base in bases:
        for d in range(-REACH, REACH + 1):
            out = jnp.where(offset + base == d, centre if d == 0 else weight_of(d), out)
    return out.astype(jnp.bfloat16)


def along_lanes(rows, weights):
    total = None
    for part in range(3):
        piece = rows.astype(jnp.bfloat16)
        rows = rows - piece.astype(jnp.float32)
        term = jnp.dot(piece, weights, preferred_element_type=jnp.float32)
        total = term if total is None else total + term
    return total


def rolled_rows(block, roll):
    rows = block.shape[1]
    return block if roll == 0 else pltpu.roll(block, rows - roll, 1)


def rows_sum(block, weights):
    total = None
    for roll, weight in enumerate(weights):
        term = weight[None] * rolled_rows(block, roll)
        total = term if total is None else total + term
    return total


def kernel(nx, ny, nz, cuts, early, fields, strength_in, out, strength, u, acc, tiles, xs, ys, packed, landed, via,
           in_sem, sent, x_recv, y_send, y_recv, z_recv, via_recv, answers, turn):
    species, cx, cy, cz = u.shape
    groups = cz // SLOT
    rows_packed = packed.shape[1]
    px, py, pz = lax.axis_index("gx"), lax.axis_index("gy"), lax.axis_index("gz")
    x_left, x_right = lax.rem(px + nx - 1, nx), lax.rem(px + 1, nx)
    y_left, y_right = lax.rem(py + ny - 1, ny), lax.rem(py + 1, ny)
    z_left, z_right = lax.rem(pz + nz - 1, nz), lax.rem(pz + 1, nz)
    y_peers = [y_right] if ny == 2 else [y_right, y_left]

    barrier = pltpu.get_barrier_semaphore()
    to_left, to_right = (px, py, z_left), (px, py, z_right)
    left_x, right_x = (x_left, py, pz), (x_right, py, pz)
    first_z, last_z = pz == 0, pz == nz - 1

    def tell(semaphore, peer):
        pl.semaphore_signal(semaphore, inc=1, device_id=peer, device_id_type=MESH)

    for peer in y_peers:
        tell(barrier, (px, peer, pz))
    odd = lax.rem(px, 2) == 1
    paired = nx % 2 == 0

    def both_x(semaphore):
        tell(semaphore, left_x)
        tell(semaphore, right_x)

    if paired:
        pl.when(odd)(lambda: both_x(barrier))
    else:
        both_x(barrier)
    pl.when(pz < nz - 1)(lambda: tell(barrier, to_right))

    spans = []
    begin = 0
    for size in cuts:
        spans.append((begin, size))
        begin += size
    load = pltpu.make_async_copy(fields, u, in_sem)
    gains = pltpu.make_async_copy(strength_in, strength, in_sem)
    load.start()

    held = early < len(cuts)
    mark = sum(cuts[:early])
    arrivals = [(0, mark)] + spans[early:]
    y_copies = []
    for k, (begin, size) in enumerate(spans):
        part = pl.ds(begin, size)
        y_copies.append([
            pltpu.make_async_remote_copy(
                src_ref=(fields if k < early else u).at[part], dst_ref=ys.at[side, part],
                send_sem=y_send.at[side] if k < early else sent, recv_sem=y_recv.at[side, max(k - early + 1, 0)],
                device_id=(px, peer, pz), device_id_type=MESH)
            for side, peer in enumerate(y_peers)])
    x_copies = [
        pltpu.make_async_remote_copy(
            src_ref=u.at[:, pl.ds(begin, REACH)], dst_ref=xs.at[side],
            send_sem=sent, recv_sem=x_recv,
            device_id=(peer, py, pz), device_id_type=MESH)
        for side, (begin, peer) in enumerate(((cx - REACH, x_right), (0, x_left)))
    ]

    relayed = held and ny == 2 and nz > 1 and nx > 2 and cx > 2 * via.shape[1]
    by_z, by_x = jnp.logical_and(px == 1, pz == 1), jnp.logical_and(px == 2, pz == 0)
    upper = py == 1
    source = jnp.logical_and(upper, jnp.logical_and(px == 1, pz == 0))
    relay = jnp.logical_or(by_z, by_x)
    relay_out = jnp.logical_and(upper, relay)
    back_z, back_x = jnp.logical_and(py == 0, by_z), jnp.logical_and(py == 0, by_x)
    turned, thick = pl.ds(*spans[early - 1]), via.shape[1]
    over_z, over_x, straight = pl.ds(0, thick), pl.ds(thick, thick), pl.ds(2 * thick, cx - 2 * thick)

    def hop(src, dst, send_sem, recv_sem, peer):
        return pltpu.make_async_remote_copy(
            src_ref=src, dst_ref=dst, send_sem=send_sem, recv_sem=recv_sem, device_id=peer, device_id_type=MESH)

    if relayed:
        across_y = (px, y_right, pz)
        direct = hop(fields.at[turned, straight], ys.at[0, turned, straight], y_send.at[0], y_recv.at[0, 0], across_y)
        out_z = hop(u.at[turned, over_z], via, y_send.at[0], via_recv, to_right)
        out_x = hop(u.at[turned, over_x], via, y_send.at[0], via_recv, right_x)
        over = hop(via, via, sent, via_recv, across_y)
        home_z = hop(via, ys.at[0, turned, over_z], sent, y_recv.at[0, 0], to_left)
        home_x = hop(via, ys.at[0, turned, over_x], sent, y_recv.at[0, 0], left_x)

    def settle(ref, semaphore):
        pltpu.make_async_copy(ref, ref, semaphore).wait()

    def start_y(rows):
        for row in rows:
            for copy in row:
                copy.start()

    def early_sent():
        for side in range(len(y_peers)):
            settle(u.at[pl.ds(0, mark)], y_send.at[side])

    greeters = (pz > 0).astype(jnp.int32) + (2 * (1 - lax.rem(px, 2)) if paired else 2)
    pl.semaphore_wait(barrier, len(y_peers) + greeters)
    if relayed:
        start_y(y_copies[:early - 1])
        pl.when(source)(direct.start)
        pl.when(jnp.logical_not(source))(lambda: start_y(y_copies[early - 1:early]))
    else:
        start_y(y_copies[:early])
    load.wait()
    gains.start()
    if held:
        at_once = jnp.logical_not(jnp.logical_or(odd, relay_out) if relayed else odd)
        pl.when(at_once)(lambda: start_y(y_copies[early:]))
    if paired:
        pl.when(jnp.logical_not(odd))(lambda: both_x(answers.at[0]))
    pl.when(pz > 0)(lambda: tell(answers.at[1], to_left))
    pl.when(last_z)(lambda: tell(answers.at[2], to_left))
    if paired:
        pl.when(odd)(lambda: pl.semaphore_wait(answers.at[0], 2))
    if relayed:
        pl.when(source)(out_x.start)
    for copy in x_copies:
        copy.start()

    lane = lax.broadcasted_iota(jnp.int32, (cx, cy, cz), 2)
    slot = lane // SLOT
    for p in range(rows_packed):
        first = p * groups
        here = min(groups, species - first)

        def pack(g, carry):
            head, tail = carry
            v = u[first + g]
            mine = slot == g
            head = jnp.where(mine, pltpu.roll(v, g * SLOT, 2), head)
            tail = jnp.where(mine, pltpu.roll(v, lax.rem((g + 1) * SLOT, cz), 2), tail)
            return head, tail

        zero = jnp.zeros((cx, cy, cz), jnp.float32)
        head, tail = each(0, here, AT_ONCE[0], pack, (zero, zero))
        packed[0, p] = head
        packed[1, p] = tail

    z_copies = [
        pltpu.make_async_remote_copy(
            src_ref=packed.at[side], dst_ref=landed.at[side],
            send_sem=sent, recv_sem=z_recv,
            device_id=(px, py, peer), device_id_type=MESH)
        for side, peer in enumerate((z_left, z_right))
    ]

    gains.wait()

    def start_right():
        pl.semaphore_wait(answers.at[1], 1)
        z_copies[1].start()

    def pass_token():
        pl.semaphore_wait(answers.at[2], 1)
        tell(answers.at[2], to_left)

    def close_ring():
        pl.semaphore_wait(answers.at[2], 1)
        tell(answers.at[1], to_left)
        z_copies[0].start()

    def end_ring():
        pl.semaphore_wait(answers.at[1], 1)
        z_copies[1].start()

    def forward(hop):
        settle(via, via_recv)
        hop.start()

    pl.when(pz < nz - 1)(start_right)
    if relayed:
        pl.when(source)(out_z.start)
    pl.when(pz > 0)(z_copies[0].start)
    pl.when(jnp.logical_and(pz > 0, pz < nz - 1))(pass_token)
    pl.when(first_z)(close_ring)

    own = [row_weights(cy, cz, r, (0,)) for r in range(cy)]
    if ny == 2:
        remote = [[row_weights(cy, cz, r, (cy, -cy)) for r in range(cy)]]
    else:
        remote = [[row_weights(cy, cz, r, (base,)) for r in range(cy)] for base in (-cy, cy)]
    inside = lane_weights(cz, (0,), 2.0 * WEIGHTS[0])
    across = lane_weights(cz, (cz, -cz), WEIGHTS[0])

    def along_own(s, _):
        v = u[s]
        total = along_lanes(v.reshape(cx * cy, cz), inside).reshape(cx, cy, cz)
        acc[s] = total + rows_sum(v, own)
        return 0

    each(0, species, AT_ONCE[1], along_own)
    pl.when(last_z)(end_ring)
    settle(landed, z_recv)

    def along_z(s, _):
        p, g = s // groups, lax.rem(s, groups)
        after = pltpu.roll(landed[0, p], lax.rem(cz - g * SLOT, cz), 2)
        before = pltpu.roll(landed[1, p], cz - (g + 1) * SLOT, 2)
        halo = jnp.where(lane < cz // 2, after, before)
        acc[s] = acc[s] + along_lanes(halo.reshape(cx * cy, cz), across).reshape(cx, cy, cz)
        return 0

    each(0, species, AT_ONCE[2], along_z)
    if relayed:
        def forward_out():
            forward(over)
            pl.when(jnp.logical_not(odd))(lambda: start_y(y_copies[early:]))

        pl.when(relay_out)(forward_out)

    def along_x(s, _):
        cells = [xs[0, s, i] for i in range(REACH)] + [u[s, i] for i in range(cx)]
        cells += [xs[1, s, i] for i in range(REACH)]
        for i in range(cx):
            total = acc[s, i]
            for d in range(1, REACH + 1):
                total = total + WEIGHTS[d] * (cells[REACH + i - d] + cells[REACH + i + d])
            acc[s, i] = total
        return 0

    def along_y(s, _):
        total = acc[s]
        for side, weights in enumerate(remote):
            total = total + rows_sum(ys[side, s], weights)
        out[s] = u[s] + (strength[s] * (1.0 / 1024.0)) * total
        return 0

    def go_on():
        pl.semaphore_wait(turn, 1)
        start_y(y_copies[early:])

    def pass_on():
        early_sent()
        tell(turn, right_x)

    if held:
        pl.when(jnp.logical_not(odd))(pass_on)
    if relayed:
        pl.when(back_x)(lambda: forward(home_x))
    settle(xs, x_recv)
    lax.fori_loop(0, species, along_x, 0)
    if held:
        pl.when(odd)(go_on)
    if relayed:
        pl.when(back_z)(lambda: forward(home_z))
    for k, (begin, size) in enumerate(arrivals):
        for side in range(len(y_peers)):
            settle(ys.at[side, pl.ds(begin, size)], y_recv.at[side, k])
        lax.fori_loop(begin, begin + size, along_y, 0)
    if held:
        pl.when(odd)(early_sent)
    else:
        early_sent()
    layers = 2 * species * REACH + 2 * rows_packed * cx + len(y_peers) * (species - mark) * cx
    if relayed:
        pl.when(relay)(lambda: settle(tiles.at[pl.ds(0, layers + via.shape[0] * thick)], sent))
        pl.when(jnp.logical_not(relay))(lambda: settle(tiles.at[pl.ds(0, layers)], sent))
    else:
        settle(tiles.at[pl.ds(0, layers)], sent)


def local(nx, ny, nz, fields, strength):
    species, cx, cy, cz = fields.shape
    cuts = CUTS if sum(CUTS) == species else (1,) * species
    pieces = len(cuts)
    early = EARLY if sum(CUTS) == species and nx % 2 == 0 else pieces
    sides = 1 if ny == 2 else 2
    groups = cz // SLOT
    rows_packed = -(-species // groups)
    block = (species, cx, cy, cz)
    layers = 2 * species * REACH + 2 * rows_packed * cx + sides * species * cx + species * DETOUR
    dma = pltpu.SemaphoreType.DMA
    return pl.pallas_call(
        functools.partial(kernel, nx, ny, nz, cuts, early),
        out_shape=pltpu.VMEM(block, jnp.float32),
        in_specs=[pl.BlockSpec(memory_space=pltpu.HBM), pl.BlockSpec(memory_space=pl.ANY)],
        out_specs=pl.BlockSpec(memory_space=pltpu.VMEM),
        scratch_shapes=[
            pltpu.SMEM((species,), jnp.float32),
            pltpu.VMEM(block, jnp.float32),
            pltpu.VMEM(block, jnp.float32),
            pltpu.VMEM((layers, cy, cz), jnp.float32),
            pltpu.VMEM((2, species, REACH, cy, cz), jnp.float32),
            pltpu.VMEM((sides,) + block, jnp.float32),
            pltpu.VMEM((2, rows_packed, cx, cy, cz), jnp.float32),
            pltpu.VMEM((2, rows_packed, cx, cy, cz), jnp.float32),
            pltpu.VMEM((cuts[early - 1], DETOUR, cy, cz), jnp.float32),
            dma,
            dma,
            dma,
            dma((sides,)),
            dma((sides, pieces - early + 1)),
            dma,
            dma,
            pltpu.SemaphoreType.REGULAR((3,)),
            pltpu.SemaphoreType.REGULAR,
        ],
        compiler_params=pltpu.CompilerParams(collective_id=0, has_side_effects=True, vmem_limit_bytes=56 * 1024 * 1024),
        name="filter_pass",
    )(fields, strength)


def solution(mesh):
    sizes = mesh.shape
    return jax.shard_map(
        functools.partial(local, sizes["gx"], sizes["gy"], sizes["gz"]),
        mesh=mesh,
        in_specs=(P(None, "gx", "gy", "gz"), P()),
        out_specs=P(None, "gx", "gy", "gz"),
        check_vma=False,
    )
```

```python
import functools
import jax
import jax.numpy as jnp
from jax import lax
from jax.experimental import pallas as pl
from jax.experimental.pallas import tpu as pltpu
from jax.sharding import PartitionSpec as P

MESH = pl.DeviceIdType.MESH
REACH = 5
SLOT = 8
WEIGHTS = [-252.0, 210.0, -120.0, 45.0, -10.0, 1.0]
CUTS = (19, 5, 7, 1)
EARLY = 2
DETOUR = 1
AT_ONCE = (8, 4, 8)


def each(begin, count, at_once, body, carry=0):
    step = at_once if count % at_once == 0 else 1

    def steps(k, carry):
        for i in range(step):
            carry = body(begin + k * step + i, carry)
        return carry

    return lax.fori_loop(0, count // step, steps, carry)


def weight_of(offset):
    return WEIGHTS[abs(offset)] if abs(offset) <= REACH else 0.0


def row_weights(rows, lanes, roll, bases):
    row = lax.broadcasted_iota(jnp.int32, (rows, lanes), 0)
    out = jnp.zeros((rows, lanes), jnp.float32)
    for i in range(rows):
        value = sum(weight_of((i + roll) % rows + base - i) for base in bases)
        if value:
            out = jnp.where(row == i, value, out)
    return out


def lane_weights(lanes, bases, centre):
    source = lax.broadcasted_iota(jnp.int32, (lanes, lanes), 0)
    offset = source - lax.broadcasted_iota(jnp.int32, (lanes, lanes), 1)
    out = jnp.zeros((lanes, lanes), jnp.float32)
    for base in bases:
        for d in range(-REACH, REACH + 1):
            out = jnp.where(offset + base == d, centre if d == 0 else weight_of(d), out)
    return out.astype(jnp.bfloat16)


def along_lanes(rows, weights):
    total = None
    for part in range(3):
        piece = rows.astype(jnp.bfloat16)
        rows = rows - piece.astype(jnp.float32)
        term = jnp.dot(piece, weights, preferred_element_type=jnp.float32)
        total = term if total is None else total + term
    return total


def rolled_rows(block, roll):
    rows = block.shape[1]
    return block if roll == 0 else pltpu.roll(block, rows - roll, 1)


def rows_sum(block, weights):
    total = None
    for roll, weight in enumerate(weights):
        term = weight[None] * rolled_rows(block, roll)
        total = term if total is None else total + term
    return total


def kernel(nx, ny, nz, cuts, early, fields, strength_in, out, strength, u, acc, tiles, xs, ys, packed, landed, via,
           in_sem, sent, x_recv, y_send, y_recv, z_recv, via_recv, answers, turn):
    species, cx, cy, cz = u.shape
    groups = cz // SLOT
    rows_packed = packed.shape[1]
    px, py, pz = lax.axis_index("gx"), lax.axis_index("gy"), lax.axis_index("gz")
    x_left, x_right = lax.rem(px + nx - 1, nx), lax.rem(px + 1, nx)
    y_left, y_right = lax.rem(py + ny - 1, ny), lax.rem(py + 1, ny)
    z_left, z_right = lax.rem(pz + nz - 1, nz), lax.rem(pz + 1, nz)
    y_peers = [y_right] if ny == 2 else [y_right, y_left]

    barrier = pltpu.get_barrier_semaphore()
    to_left, to_right = (px, py, z_left), (px, py, z_right)
    left_x, right_x = (x_left, py, pz), (x_right, py, pz)
    first_z, last_z = pz == 0, pz == nz - 1

    def tell(semaphore, peer):
        pl.semaphore_signal(semaphore, inc=1, device_id=peer, device_id_type=MESH)

    for peer in y_peers:
        tell(barrier, (px, peer, pz))
    odd = lax.rem(px, 2) == 1
    paired = nx % 2 == 0

    def both_x(semaphore):
        tell(semaphore, left_x)
        tell(semaphore, right_x)

    if paired:
        pl.when(odd)(lambda: both_x(barrier))
    else:
        both_x(barrier)
    pl.when(pz < nz - 1)(lambda: tell(barrier, to_right))

    spans = []
    begin = 0
    for size in cuts:
        spans.append((begin, size))
        begin += size
    load = pltpu.make_async_copy(fields, u, in_sem)
    gains = pltpu.make_async_copy(strength_in, strength, in_sem)
    load.start()

    held = early < len(cuts)
    mark = sum(cuts[:early])
    y_copies = []
    for k, (begin, size) in enumerate(spans):
        part = pl.ds(begin, size)
        y_copies.append([
            pltpu.make_async_remote_copy(
                src_ref=(fields if k < early else u).at[part], dst_ref=ys.at[side, part],
                send_sem=y_send.at[side] if k < early else sent, recv_sem=y_recv.at[side, k],
                device_id=(px, peer, pz), device_id_type=MESH)
            for side, peer in enumerate(y_peers)])
    x_copies = [
        pltpu.make_async_remote_copy(
            src_ref=u.at[:, pl.ds(begin, REACH)], dst_ref=xs.at[side],
            send_sem=sent, recv_sem=x_recv,
            device_id=(peer, py, pz), device_id_type=MESH)
        for side, (begin, peer) in enumerate(((cx - REACH, x_right), (0, x_left)))
    ]

    relayed = held and ny == 2 and nz > 1 and nx > 2 and cx > 2 * via.shape[1]
    by_z, by_x = jnp.logical_and(px == 1, pz == 1), jnp.logical_and(px == 2, pz == 0)
    upper = py == 1
    source = jnp.logical_and(upper, jnp.logical_and(px == 1, pz == 0))
    relay = jnp.logical_or(by_z, by_x)
    relay_out = jnp.logical_and(upper, relay)
    back_z, back_x = jnp.logical_and(py == 0, by_z), jnp.logical_and(py == 0, by_x)
    turned, thick = pl.ds(*spans[early - 1]), via.shape[1]
    over_z, over_x, straight = pl.ds(0, thick), pl.ds(thick, thick), pl.ds(2 * thick, cx - 2 * thick)

    def hop(src, dst, send_sem, recv_sem, peer):
        return pltpu.make_async_remote_copy(
            src_ref=src, dst_ref=dst, send_sem=send_sem, recv_sem=recv_sem, device_id=peer, device_id_type=MESH)

    if relayed:
        across_y = (px, y_right, pz)
        direct = hop(fields.at[turned, straight], ys.at[0, turned, straight], y_send.at[0], y_recv.at[0, early - 1], across_y)
        out_z = hop(u.at[turned, over_z], via, y_send.at[0], via_recv, to_right)
        out_x = hop(u.at[turned, over_x], via, y_send.at[0], via_recv, right_x)
        over = hop(via, via, sent, via_recv, across_y)
        home_z = hop(via, ys.at[0, turned, over_z], sent, y_recv.at[0, early - 1], to_left)
        home_x = hop(via, ys.at[0, turned, over_x], sent, y_recv.at[0, early - 1], left_x)

    def settle(ref, semaphore):
        pltpu.make_async_copy(ref, ref, semaphore).wait()

    def start_y(rows):
        for row in rows:
            for copy in row:
                copy.start()

    def early_sent():
        for side in range(len(y_peers)):
            settle(u.at[pl.ds(0, mark)], y_send.at[side])

    greeters = (pz > 0).astype(jnp.int32) + (2 * (1 - lax.rem(px, 2)) if paired else 2)
    pl.semaphore_wait(barrier, len(y_peers) + greeters)
    if relayed:
        start_y(y_copies[:early - 1])
        pl.when(source)(direct.start)
        pl.when(jnp.logical_not(source))(lambda: start_y(y_copies[early - 1:early]))
    else:
        start_y(y_copies[:early])
    load.wait()
    gains.start()
    if held:
        at_once = jnp.logical_not(jnp.logical_or(odd, relay_out) if relayed else odd)
        pl.when(at_once)(lambda: start_y(y_copies[early:]))
    if paired:
        pl.when(jnp.logical_not(odd))(lambda: both_x(answers.at[0]))
    pl.when(pz > 0)(lambda: tell(answers.at[1], to_left))
    pl.when(last_z)(lambda: tell(answers.at[2], to_left))
    if paired:
        pl.when(odd)(lambda: pl.semaphore_wait(answers.at[0], 2))
    if relayed:
        pl.when(source)(out_x.start)
    for copy in x_copies:
        copy.start()

    lane = lax.broadcasted_iota(jnp.int32, (cx, cy, cz), 2)
    slot = lane // SLOT
    for p in range(rows_packed):
        first = p * groups
        here = min(groups, species - first)

        def pack(g, carry):
            head, tail = carry
            v = u[first + g]
            mine = slot == g
            head = jnp.where(mine, pltpu.roll(v, g * SLOT, 2), head)
            tail = jnp.where(mine, pltpu.roll(v, lax.rem((g + 1) * SLOT, cz), 2), tail)
            return head, tail

        zero = jnp.zeros((cx, cy, cz), jnp.float32)
        head, tail = each(0, here, AT_ONCE[0], pack, (zero, zero))
        packed[0, p] = head
        packed[1, p] = tail

    z_copies = [
        pltpu.make_async_remote_copy(
            src_ref=packed.at[side], dst_ref=landed.at[side],
            send_sem=sent, recv_sem=z_recv,
            device_id=(px, py, peer), device_id_type=MESH)
        for side, peer in enumerate((z_left, z_right))
    ]

    gains.wait()

    def start_right():
        pl.semaphore_wait(answers.at[1], 1)
        z_copies[1].start()

    def pass_token():
        pl.semaphore_wait(answers.at[2], 1)
        tell(answers.at[2], to_left)

    def close_ring():
        pl.semaphore_wait(answers.at[2], 1)
        tell(answers.at[1], to_left)
        z_copies[0].start()

    def end_ring():
        pl.semaphore_wait(answers.at[1], 1)
        z_copies[1].start()

    def forward(hop):
        settle(via, via_recv)
        hop.start()

    pl.when(pz < nz - 1)(start_right)
    if relayed:
        pl.when(source)(out_z.start)
    pl.when(pz > 0)(z_copies[0].start)
    pl.when(jnp.logical_and(pz > 0, pz < nz - 1))(pass_token)
    pl.when(first_z)(close_ring)

    own = [row_weights(cy, cz, r, (0,)) for r in range(cy)]
    if ny == 2:
        remote = [[row_weights(cy, cz, r, (cy, -cy)) for r in range(cy)]]
    else:
        remote = [[row_weights(cy, cz, r, (base,)) for r in range(cy)] for base in (-cy, cy)]
    inside = lane_weights(cz, (0,), 2.0 * WEIGHTS[0])
    across = lane_weights(cz, (cz, -cz), WEIGHTS[0])

    def along_own(s, _):
        v = u[s]
        total = along_lanes(v.reshape(cx * cy, cz), inside).reshape(cx, cy, cz)
        acc[s] = total + rows_sum(v, own)
        return 0

    each(0, species, AT_ONCE[1], along_own)
    pl.when(last_z)(end_ring)
    settle(landed, z_recv)

    def along_z(s, _):
        p, g = s // groups, lax.rem(s, groups)
        after = pltpu.roll(landed[0, p], lax.rem(cz - g * SLOT, cz), 2)
        before = pltpu.roll(landed[1, p], cz - (g + 1) * SLOT, 2)
        halo = jnp.where(lane < cz // 2, after, before)
        acc[s] = acc[s] + along_lanes(halo.reshape(cx * cy, cz), across).reshape(cx, cy, cz)
        return 0

    each(0, species, AT_ONCE[2], along_z)
    if relayed:
        def forward_out():
            forward(over)
            pl.when(jnp.logical_not(odd))(lambda: start_y(y_copies[early:]))

        pl.when(relay_out)(forward_out)

    def along_x(s, _):
        cells = [xs[0, s, i] for i in range(REACH)] + [u[s, i] for i in range(cx)]
        cells += [xs[1, s, i] for i in range(REACH)]
        for i in range(cx):
            total = acc[s, i]
            for d in range(1, REACH + 1):
                total = total + WEIGHTS[d] * (cells[REACH + i - d] + cells[REACH + i + d])
            acc[s, i] = total
        return 0

    def along_y(s, _):
        total = acc[s]
        for side, weights in enumerate(remote):
            total = total + rows_sum(ys[side, s], weights)
        out[s] = u[s] + (strength[s] * (1.0 / 1024.0)) * total
        return 0

    def go_on():
        pl.semaphore_wait(turn, 1)
        start_y(y_copies[early:])

    def pass_on():
        early_sent()
        tell(turn, right_x)

    if held:
        pl.when(jnp.logical_not(odd))(pass_on)
    if relayed:
        pl.when(back_x)(lambda: forward(home_x))
    settle(xs, x_recv)
    lax.fori_loop(0, species, along_x, 0)
    if held:
        pl.when(odd)(go_on)
    if relayed:
        pl.when(back_z)(lambda: forward(home_z))
    for k, (begin, size) in enumerate(spans):
        for side in range(len(y_peers)):
            settle(ys.at[side, pl.ds(begin, size)], y_recv.at[side, k])
        lax.fori_loop(begin, begin + size, along_y, 0)
    if held:
        pl.when(odd)(early_sent)
    else:
        early_sent()
    layers = 2 * species * REACH + 2 * rows_packed * cx + len(y_peers) * (species - mark) * cx
    if relayed:
        pl.when(relay)(lambda: settle(tiles.at[pl.ds(0, layers + via.shape[0] * thick)], sent))
        pl.when(jnp.logical_not(relay))(lambda: settle(tiles.at[pl.ds(0, layers)], sent))
    else:
        settle(tiles.at[pl.ds(0, layers)], sent)


def local(nx, ny, nz, fields, strength):
    species, cx, cy, cz = fields.shape
    cuts = CUTS if sum(CUTS) == species else (1,) * species
    pieces = len(cuts)
    early = EARLY if sum(CUTS) == species and nx % 2 == 0 else pieces
    sides = 1 if ny == 2 else 2
    groups = cz // SLOT
    rows_packed = -(-species // groups)
    block = (species, cx, cy, cz)
    layers = 2 * species * REACH + 2 * rows_packed * cx + sides * species * cx + species * DETOUR
    dma = pltpu.SemaphoreType.DMA
    return pl.pallas_call(
        functools.partial(kernel, nx, ny, nz, cuts, early),
        out_shape=pltpu.VMEM(block, jnp.float32),
        in_specs=[pl.BlockSpec(memory_space=pltpu.HBM), pl.BlockSpec(memory_space=pl.ANY)],
        out_specs=pl.BlockSpec(memory_space=pltpu.VMEM),
        scratch_shapes=[
            pltpu.SMEM((species,), jnp.float32),
            pltpu.VMEM(block, jnp.float32),
            pltpu.VMEM(block, jnp.float32),
            pltpu.VMEM((layers, cy, cz), jnp.float32),
            pltpu.VMEM((2, species, REACH, cy, cz), jnp.float32),
            pltpu.VMEM((sides,) + block, jnp.float32),
            pltpu.VMEM((2, rows_packed, cx, cy, cz), jnp.float32),
            pltpu.VMEM((2, rows_packed, cx, cy, cz), jnp.float32),
            pltpu.VMEM((cuts[early - 1], DETOUR, cy, cz), jnp.float32),
            dma,
            dma,
            dma,
            dma((sides,)),
            dma((sides, pieces)),
            dma,
            dma,
            pltpu.SemaphoreType.REGULAR((3,)),
            pltpu.SemaphoreType.REGULAR,
        ],
        compiler_params=pltpu.CompilerParams(collective_id=0, has_side_effects=True, vmem_limit_bytes=56 * 1024 * 1024),
        name="filter_pass",
    )(fields, strength)


def solution(mesh):
    sizes = mesh.shape
    return jax.shard_map(
        functools.partial(local, sizes["gx"], sizes["gy"], sizes["gz"]),
        mesh=mesh,
        in_specs=(P(None, "gx", "gy", "gz"), P()),
        out_specs=P(None, "gx", "gy", "gz"),
        check_vma=False,
    )
```

```python
import functools
import jax
import jax.numpy as jnp
from jax import lax
from jax.experimental import pallas as pl
from jax.experimental.pallas import tpu as pltpu
from jax.sharding import PartitionSpec as P

MESH = pl.DeviceIdType.MESH
REACH = 5
SLOT = 8
WEIGHTS = [-252.0, 210.0, -120.0, 45.0, -10.0, 1.0]
CUTS = (16, 5, 3, 2, 5, 1)
EARLY = 2
LATE = 2
AT_ONCE = (8, 4, 8)


def each(begin, count, at_once, body, carry=0):
    step = at_once if count % at_once == 0 else 1

    def steps(k, carry):
        for i in range(step):
            carry = body(begin + k * step + i, carry)
        return carry

    return lax.fori_loop(0, count // step, steps, carry)


def weight_of(offset):
    return WEIGHTS[abs(offset)] if abs(offset) <= REACH else 0.0


def row_weights(rows, lanes, roll, bases):
    row = lax.broadcasted_iota(jnp.int32, (rows, lanes), 0)
    out = jnp.zeros((rows, lanes), jnp.float32)
    for i in range(rows):
        value = sum(weight_of((i + roll) % rows + base - i) for base in bases)
        if value:
            out = jnp.where(row == i, value, out)
    return out


def lane_weights(lanes, bases, centre):
    source = lax.broadcasted_iota(jnp.int32, (lanes, lanes), 0)
    offset = source - lax.broadcasted_iota(jnp.int32, (lanes, lanes), 1)
    out = jnp.zeros((lanes, lanes), jnp.float32)
    for base in bases:
        for d in range(-REACH, REACH + 1):
            out = jnp.where(offset + base == d, centre if d == 0 else weight_of(d), out)
    return out.astype(jnp.bfloat16)


def along_lanes(rows, weights):
    total = None
    for part in range(3):
        piece = rows.astype(jnp.bfloat16)
        rows = rows - piece.astype(jnp.float32)
        term = jnp.dot(piece, weights, preferred_element_type=jnp.float32)
        total = term if total is None else total + term
    return total


def rolled_rows(block, roll):
    rows = block.shape[1]
    return block if roll == 0 else pltpu.roll(block, rows - roll, 1)


def rows_sum(block, weights):
    total = None
    for roll, weight in enumerate(weights):
        term = weight[None] * rolled_rows(block, roll)
        total = term if total is None else total + term
    return total


def kernel(nx, ny, nz, cuts, early, late, fields, strength_in, out, late_u, late_gain, strength, u, acc, tiles, xs, ys, packed, landed,
           in_sem, sent, x_recv, y_send, y_recv, z_recv, answers, turn):
    species, cx, cy, cz = u.shape
    groups = cz // SLOT
    rows_packed = packed.shape[1]
    px, py, pz = lax.axis_index("gx"), lax.axis_index("gy"), lax.axis_index("gz")
    x_left, x_right = lax.rem(px + nx - 1, nx), lax.rem(px + 1, nx)
    y_left, y_right = lax.rem(py + ny - 1, ny), lax.rem(py + 1, ny)
    z_left, z_right = lax.rem(pz + nz - 1, nz), lax.rem(pz + 1, nz)
    y_peers = [y_right] if ny == 2 else [y_right, y_left]

    barrier = pltpu.get_barrier_semaphore()
    to_left, to_right = (px, py, z_left), (px, py, z_right)
    left_x, right_x = (x_left, py, pz), (x_right, py, pz)
    first_z, last_z = pz == 0, pz == nz - 1

    def tell(semaphore, peer):
        pl.semaphore_signal(semaphore, inc=1, device_id=peer, device_id_type=MESH)

    for peer in y_peers:
        tell(barrier, (px, peer, pz))
    odd = lax.rem(px, 2) == 1
    paired = nx % 2 == 0

    def both_x(semaphore):
        tell(semaphore, left_x)
        tell(semaphore, right_x)

    if paired:
        pl.when(odd)(lambda: both_x(barrier))
    else:
        both_x(barrier)
    pl.when(pz < nz - 1)(lambda: tell(barrier, to_right))

    spans = []
    begin = 0
    for size in cuts:
        spans.append((begin, size))
        begin += size
    load = pltpu.make_async_copy(fields, u, in_sem)
    late_load = pltpu.make_async_copy(fields.at[pl.ds(species - late, late)], late_u, in_sem) if late else None
    gains = pltpu.make_async_copy(strength_in, strength, in_sem)
    load.start()

    held = early < len(cuts)
    mark = sum(cuts[:early + 1])
    kept = species - late
    y_copies = []
    for k, (begin, size) in enumerate(spans):
        part = pl.ds(begin, size)
        y_copies.append([
            pltpu.make_async_remote_copy(
                src_ref=(fields if k < early else u).at[part], dst_ref=ys.at[side, part],
                send_sem=y_send.at[side] if begin < mark else sent, recv_sem=y_recv.at[side, k],
                device_id=(px, peer, pz), device_id_type=MESH)
            for side, peer in enumerate(y_peers)])
    x_spans = [(0, cuts[0]), (cuts[0], species - cuts[0])]
    x_copies = [
        pltpu.make_async_remote_copy(
            src_ref=u.at[pl.ds(*span), pl.ds(begin, REACH)], dst_ref=xs.at[pl.ds(*span), side],
            send_sem=sent, recv_sem=x_recv.at[k],
            device_id=(peer, py, pz), device_id_type=MESH)
        for k, span in enumerate(x_spans)
        for side, (begin, peer) in enumerate(((cx - REACH, x_right), (0, x_left)))
    ]

    def settle(ref, semaphore):
        pltpu.make_async_copy(ref, ref, semaphore).wait()

    def start_y(rows):
        for row in rows:
            for copy in row:
                copy.start()

    def early_sent():
        for side in range(len(y_peers)):
            settle(u.at[pl.ds(0, mark)], y_send.at[side])

    greeters = (pz > 0).astype(jnp.int32) + (2 * (1 - lax.rem(px, 2)) if paired else 2)
    pl.semaphore_wait(barrier, len(y_peers) + greeters)
    start_y(y_copies[:early])
    load.wait()
    gains.start()
    if held:
        pl.when(odd)(lambda: start_y(y_copies[early:-LATE]))
    if paired:
        pl.when(jnp.logical_not(odd))(lambda: both_x(answers.at[0]))
    pl.when(pz > 0)(lambda: tell(answers.at[1], to_left))
    pl.when(last_z)(lambda: tell(answers.at[2], to_left))
    if paired:
        pl.when(odd)(lambda: pl.semaphore_wait(answers.at[0], 2))
    for k in range(0, len(x_copies), 2):
        if held:
            pl.when(jnp.logical_not(odd))(x_copies[k].start)
        else:
            x_copies[k].start()
        x_copies[k + 1].start()

    lane = lax.broadcasted_iota(jnp.int32, (cx, cy, cz), 2)
    slot = lane // SLOT
    for p in range(rows_packed):
        first = p * groups
        here = min(groups, species - first)

        def pack(g, carry):
            head, tail = carry
            v = u[first + g]
            mine = slot == g
            head = jnp.where(mine, pltpu.roll(v, g * SLOT, 2), head)
            tail = jnp.where(mine, pltpu.roll(v, lax.rem((g + 1) * SLOT, cz), 2), tail)
            return head, tail

        zero = jnp.zeros((cx, cy, cz), jnp.float32)
        head, tail = each(0, here, AT_ONCE[0], pack, (zero, zero))
        packed[0, p] = head
        packed[1, p] = tail

    z_copies = [
        pltpu.make_async_remote_copy(
            src_ref=packed.at[side], dst_ref=landed.at[side],
            send_sem=sent, recv_sem=z_recv,
            device_id=(px, py, peer), device_id_type=MESH)
        for side, peer in enumerate((z_left, z_right))
    ]

    gains.wait()
    if held:
        late_load.start()
        for i in range(late):
            late_gain[i] = jnp.zeros((cy, cz), jnp.float32) + strength[kept + i] * (1.0 / 1024.0)

    def start_right():
        pl.semaphore_wait(answers.at[1], 1)
        z_copies[1].start()

    def pass_token():
        pl.semaphore_wait(answers.at[2], 1)
        tell(answers.at[2], to_left)

    def close_ring():
        pl.semaphore_wait(answers.at[2], 1)
        tell(answers.at[1], to_left)
        z_copies[0].start()

    def end_ring():
        pl.semaphore_wait(answers.at[1], 1)
        z_copies[1].start()

    pl.when(pz < nz - 1)(start_right)
    pl.when(pz > 0)(z_copies[0].start)
    pl.when(jnp.logical_and(pz > 0, pz < nz - 1))(pass_token)
    pl.when(first_z)(close_ring)

    own = [row_weights(cy, cz, r, (0,)) for r in range(cy)]
    if ny == 2:
        remote = [[row_weights(cy, cz, r, (cy, -cy)) for r in range(cy)]]
    else:
        remote = [[row_weights(cy, cz, r, (base,)) for r in range(cy)] for base in (-cy, cy)]
    inside = lane_weights(cz, (0,), 2.0 * WEIGHTS[0])
    across = lane_weights(cz, (cz, -cz), WEIGHTS[0])

    def along_own(s, _):
        v = u[s]
        total = along_lanes(v.reshape(cx * cy, cz), inside).reshape(cx, cy, cz)
        acc[s] = total + rows_sum(v, own)
        return 0

    each(0, species, AT_ONCE[1], along_own)
    if held:
        def start_held():
            for copy in x_copies[0::2]:
                copy.start()

        pl.when(odd)(start_held)
    pl.when(last_z)(end_ring)
    settle(landed, z_recv)

    def along_z(s, _):
        p, g = s // groups, lax.rem(s, groups)
        after = pltpu.roll(landed[0, p], lax.rem(cz - g * SLOT, cz), 2)
        before = pltpu.roll(landed[1, p], cz - (g + 1) * SLOT, 2)
        halo = jnp.where(lane < cz // 2, after, before)
        acc[s] = acc[s] + along_lanes(halo.reshape(cx * cy, cz), across).reshape(cx, cy, cz)
        return 0

    each(0, species, AT_ONCE[2], along_z)

    def along_x(s, _):
        gain = strength[s] * (1.0 / 1024.0)
        cells = [xs[s, 0, i] for i in range(REACH)] + [u[s, i] for i in range(cx)]
        cells += [xs[s, 1, i] for i in range(REACH)]
        for i in range(cx):
            total = acc[s, i]
            for d in range(1, REACH + 1):
                total = total + WEIGHTS[d] * (cells[REACH + i - d] + cells[REACH + i + d])
            acc[s, i] = total
            out[s, i] = cells[REACH + i] + gain * total
        return 0

    def from_y(s):
        total = acc[s]
        for side, weights in enumerate(remote):
            total = total + rows_sum(ys[side, s], weights)
        return total

    def along_y(s, _):
        acc[s] = from_y(s)
        return 0

    def along_last(s, _):
        out[s] = u[s] + (strength[s] * (1.0 / 1024.0)) * from_y(s)
        return 0

    def go_on():
        pl.semaphore_wait(turn, 1)
        start_y(y_copies[early:])

    def pass_on():
        early_sent()
        tell(turn, left_x)

    def add_y(k, body):
        begin, size = spans[k]
        for side in range(len(y_peers)):
            settle(ys.at[side, pl.ds(begin, size)], y_recv.at[side, k])
        lax.fori_loop(begin, begin + size, body, 0)

    def add_x(k):
        begin, size = x_spans[k]
        settle(xs.at[pl.ds(begin, size)], x_recv.at[k])
        lax.fori_loop(begin, begin + size, along_x, 0)

    def rest():
        for k in range(len(spans) - LATE, len(spans)):
            add_y(k, along_last)

    add_y(0, along_y)
    add_x(0)
    if held:
        pl.when(odd)(pass_on)
        pl.when(jnp.logical_not(odd))(go_on)
        for k in range(1, early + 1):
            add_y(k, along_y)
        add_x(1)
        for k in range(early + 1, len(spans) - LATE):
            add_y(k, along_last)
        late_load.wait()
        pl.when(jnp.logical_not(odd))(rest)
        pl.when(jnp.logical_not(odd))(early_sent)
    else:
        add_x(1)
        for k in range(1, len(spans)):
            add_y(k, along_last)
        early_sent()
    layers = 2 * species * REACH + 2 * rows_packed * cx
    tails = [(None, 0)]
    if held:
        sides = len(y_peers)
        tails = [(odd, sides * (kept - mark) * cx), (jnp.logical_not(odd), sides * (species - mark) * cx)]
    for who, count in tails:
        last = functools.partial(settle, tiles.at[pl.ds(0, layers + count)], sent)
        if who is None:
            last()
        else:
            pl.when(who)(last)


def late_kernel(ny, cuts, filtered, late_u, late_gain, _, late_out, ys, send, recv):
    late, cx, cy, cz = late_u.shape
    px, py, pz = lax.axis_index("gx"), lax.axis_index("gy"), lax.axis_index("gz")
    y_left, y_right = lax.rem(py + ny - 1, ny), lax.rem(py + 1, ny)
    y_peers = [y_right] if ny == 2 else [y_right, y_left]
    kept = filtered.shape[0] - late

    def exchange():
        barrier = pltpu.get_barrier_semaphore()
        for peer in y_peers:
            pl.semaphore_signal(barrier, inc=1, device_id=(px, peer, pz), device_id_type=MESH)
        pl.semaphore_wait(barrier, len(y_peers))
        copies = []
        begin = 0
        for k, size in enumerate(cuts):
            part = pl.ds(begin, size)
            copies.append([
                pltpu.make_async_remote_copy(
                    src_ref=late_u.at[part], dst_ref=ys.at[side, part], send_sem=send.at[side], recv_sem=recv.at[side, k],
                    device_id=(px, peer, pz), device_id_type=MESH)
                for side, peer in enumerate(y_peers)])
            begin += size
        for row in copies:
            for copy in row:
                copy.start()
        if ny == 2:
            remote = [[row_weights(cy, cz, r, (cy, -cy)) for r in range(cy)]]
        else:
            remote = [[row_weights(cy, cz, r, (base,)) for r in range(cy)] for base in (-cy, cy)]
        s = 0
        for size, row in zip(cuts, copies):
            for copy in row:
                copy.wait_recv()
            for s in range(s, s + size):
                total = None
                for side, weights in enumerate(remote):
                    term = rows_sum(ys[side, s], weights)
                    total = term if total is None else total + term
                late_out[s] = filtered[kept + s] + late_gain[s][None] * total
            s += 1
        for side in range(len(y_peers)):
            pltpu.make_async_copy(late_u, late_u, send.at[side]).wait()

    pl.when(lax.rem(px, 2) == 1)(exchange)


def write_kernel(late, filtered, out, token, done):
    species = filtered.shape[0]

    def write(count):
        part = pl.ds(0, count)
        copy = pltpu.make_async_copy(filtered.at[part], out.at[part], done)
        copy.start()
        copy.wait()

    odd = lax.rem(lax.axis_index("gx"), 2) == 1
    pl.when(odd)(lambda: write(species - late))
    pl.when(jnp.logical_not(odd))(lambda: write(species))
    token[...] = jnp.zeros(token.shape, token.dtype)


def close_kernel(_, late_out, out, done):
    late, species = late_out.shape[0], out.shape[0]

    def write():
        copy = pltpu.make_async_copy(late_out, out.at[pl.ds(species - late, late)], done)
        copy.start()
        copy.wait()

    pl.when(lax.rem(lax.axis_index("gx"), 2) == 1)(write)


def local(nx, ny, nz, fields, strength):
    species, cx, cy, cz = fields.shape
    cuts = CUTS if sum(CUTS) == species else (1,) * species
    pieces = len(cuts)
    early = EARLY if sum(CUTS) == species and nx % 2 == 0 else pieces
    sides = 1 if ny == 2 else 2
    groups = cz // SLOT
    rows_packed = -(-species // groups)
    block = (species, cx, cy, cz)
    layers = 2 * species * REACH + 2 * rows_packed * cx + sides * species * cx
    dma = pltpu.SemaphoreType.DMA
    late = sum(cuts[-LATE:])
    filtered, late_u, late_gain = pl.pallas_call(
        functools.partial(kernel, nx, ny, nz, cuts, early, late),
        out_shape=(pltpu.VMEM(block, jnp.float32), pltpu.VMEM((late,) + block[1:], jnp.float32),
                   pltpu.VMEM((late, cy, cz), jnp.float32)),
        in_specs=[pl.BlockSpec(memory_space=pltpu.HBM), pl.BlockSpec(memory_space=pl.ANY)],
        out_specs=(pl.BlockSpec(memory_space=pltpu.VMEM),) * 3,
        scratch_shapes=[
            pltpu.SMEM((species,), jnp.float32),
            pltpu.VMEM(block, jnp.float32),
            pltpu.VMEM(block, jnp.float32),
            pltpu.VMEM((layers, cy, cz), jnp.float32),
            pltpu.VMEM((species, 2, REACH, cy, cz), jnp.float32),
            pltpu.VMEM((sides,) + block, jnp.float32),
            pltpu.VMEM((2, rows_packed, cx, cy, cz), jnp.float32),
            pltpu.VMEM((2, rows_packed, cx, cy, cz), jnp.float32),
            dma,
            dma,
            dma((2,)),
            dma((sides,)),
            dma((sides, pieces)),
            dma,
            pltpu.SemaphoreType.REGULAR((3,)),
            pltpu.SemaphoreType.REGULAR,
        ],
        compiler_params=pltpu.CompilerParams(collective_id=0, has_side_effects=True, vmem_limit_bytes=56 * 1024 * 1024),
        name="filter_pass",
    )(fields, strength)
    if early == pieces:
        return filtered
    vmem, hbm = pl.BlockSpec(memory_space=pltpu.VMEM), pl.BlockSpec(memory_space=pltpu.HBM)
    small = 4 * 1024 * 1024
    written, token = pl.pallas_call(
        functools.partial(write_kernel, late),
        out_shape=(pltpu.HBM(block, jnp.float32), pltpu.VMEM((8, 128), jnp.float32)),
        in_specs=[vmem], out_specs=(hbm, vmem), scratch_shapes=[dma],
        compiler_params=pltpu.CompilerParams(vmem_limit_bytes=small), name="write",
    )(filtered)
    late_out = pl.pallas_call(
        functools.partial(late_kernel, ny, cuts[-LATE:]),
        out_shape=pltpu.VMEM((late,) + block[1:], jnp.float32),
        in_specs=[vmem] * 4, out_specs=vmem,
        scratch_shapes=[pltpu.VMEM((sides, late) + block[1:], jnp.float32), dma((sides,)), dma((sides, LATE))],
        compiler_params=pltpu.CompilerParams(collective_id=1, has_side_effects=True, vmem_limit_bytes=small), name="late",
    )(filtered, late_u, late_gain, token)
    return pl.pallas_call(
        close_kernel,
        out_shape=pltpu.HBM(block, jnp.float32),
        in_specs=[hbm, vmem], out_specs=hbm, scratch_shapes=[dma], input_output_aliases={0: 0},
        compiler_params=pltpu.CompilerParams(vmem_limit_bytes=small), name="close",
    )(written, late_out)


def solution(mesh):
    sizes = mesh.shape
    return jax.shard_map(
        functools.partial(local, sizes["gx"], sizes["gy"], sizes["gz"]),
        mesh=mesh,
        in_specs=(P(None, "gx", "gy", "gz"), P()),
        out_specs=P(None, "gx", "gy", "gz"),
        check_vma=False,
    )
```

```python
import functools
import jax
import jax.numpy as jnp
from jax import lax
from jax.experimental import pallas as pl
from jax.experimental.pallas import tpu as pltpu
from jax.sharding import PartitionSpec as P

MESH = pl.DeviceIdType.MESH
REACH = 5
SLOT = 8
WEIGHTS = [-252.0, 210.0, -120.0, 45.0, -10.0, 1.0]
CUTS = (19, 5, 7, 1)
EARLY = 2
DETOUR = 1
AT_ONCE = (8, 4, 8)


def each(begin, count, at_once, body, carry=0):
    step = at_once if count % at_once == 0 else 1

    def steps(k, carry):
        for i in range(step):
            carry = body(begin + k * step + i, carry)
        return carry

    return lax.fori_loop(0, count // step, steps, carry)


def weight_of(offset):
    return WEIGHTS[abs(offset)] if abs(offset) <= REACH else 0.0


def row_weights(rows, lanes, roll, bases):
    row = lax.broadcasted_iota(jnp.int32, (rows, lanes), 0)
    out = jnp.zeros((rows, lanes), jnp.float32)
    for i in range(rows):
        value = sum(weight_of((i + roll) % rows + base - i) for base in bases)
        if value:
            out = jnp.where(row == i, value, out)
    return out


def lane_weights(lanes, bases, centre):
    source = lax.broadcasted_iota(jnp.int32, (lanes, lanes), 0)
    offset = source - lax.broadcasted_iota(jnp.int32, (lanes, lanes), 1)
    out = jnp.zeros((lanes, lanes), jnp.float32)
    for base in bases:
        for d in range(-REACH, REACH + 1):
            out = jnp.where(offset + base == d, centre if d == 0 else weight_of(d), out)
    return out.astype(jnp.bfloat16)


def along_lanes(rows, weights):
    total = None
    for part in range(3):
        piece = rows.astype(jnp.bfloat16)
        rows = rows - piece.astype(jnp.float32)
        term = jnp.dot(piece, weights, preferred_element_type=jnp.float32)
        total = term if total is None else total + term
    return total


def rolled_rows(block, roll):
    rows = block.shape[1]
    return block if roll == 0 else pltpu.roll(block, rows - roll, 1)


def rows_sum(block, weights):
    total = None
    for roll, weight in enumerate(weights):
        term = weight[None] * rolled_rows(block, roll)
        total = term if total is None else total + term
    return total


def kernel(nx, ny, nz, cuts, early, fields, strength_in, out, strength, u, acc, tiles, xs, ys, packed, landed, via,
           in_sem, sent, x_recv, y_send, y_recv, z_recv, via_recv, answers, turn):
    species, cx, cy, cz = u.shape
    groups = cz // SLOT
    rows_packed = packed.shape[1]
    px, py, pz = lax.axis_index("gx"), lax.axis_index("gy"), lax.axis_index("gz")
    x_left, x_right = lax.rem(px + nx - 1, nx), lax.rem(px + 1, nx)
    y_left, y_right = lax.rem(py + ny - 1, ny), lax.rem(py + 1, ny)
    z_left, z_right = lax.rem(pz + nz - 1, nz), lax.rem(pz + 1, nz)
    y_peers = [y_right] if ny == 2 else [y_right, y_left]

    barrier = pltpu.get_barrier_semaphore()
    to_left, to_right = (px, py, z_left), (px, py, z_right)
    left_x, right_x = (x_left, py, pz), (x_right, py, pz)
    first_z, last_z = pz == 0, pz == nz - 1

    def tell(semaphore, peer):
        pl.semaphore_signal(semaphore, inc=1, device_id=peer, device_id_type=MESH)

    for peer in y_peers:
        tell(barrier, (px, peer, pz))
    odd = lax.rem(px, 2) == 1
    paired = nx % 2 == 0

    def both_x(semaphore):
        tell(semaphore, left_x)
        tell(semaphore, right_x)

    if paired:
        pl.when(odd)(lambda: both_x(barrier))
    else:
        both_x(barrier)
    pl.when(pz < nz - 1)(lambda: tell(barrier, to_right))

    spans = []
    begin = 0
    for size in cuts:
        spans.append((begin, size))
        begin += size
    load = pltpu.make_async_copy(fields, u, in_sem)
    gains = pltpu.make_async_copy(strength_in, strength, in_sem)
    load.start()

    held = early < len(cuts)
    mark = sum(cuts[:early])

    def y_row(k, source):
        part = pl.ds(*spans[k])
        return [
            pltpu.make_async_remote_copy(
                src_ref=source.at[part], dst_ref=ys.at[side, part],
                send_sem=y_send.at[side] if k < early else sent, recv_sem=y_recv.at[side, k],
                device_id=(px, peer, pz), device_id_type=MESH)
            for side, peer in enumerate(y_peers)]

    y_copies = [y_row(k, fields if k < early else u) for k in range(len(spans))]
    loaded_copies = [y_row(k, u) for k in range(early)]
    x_copies = [
        pltpu.make_async_remote_copy(
            src_ref=u.at[:, pl.ds(begin, REACH)], dst_ref=xs.at[side],
            send_sem=sent, recv_sem=x_recv,
            device_id=(peer, py, pz), device_id_type=MESH)
        for side, (begin, peer) in enumerate(((cx - REACH, x_right), (0, x_left)))
    ]

    relayed = held and ny == 2 and nz > 1 and nx > 2 and cx > 2 * via.shape[1]
    by_z, by_x = jnp.logical_and(px == 1, pz == 1), jnp.logical_and(px == 2, pz == 0)
    upper = py == 1
    source = jnp.logical_and(upper, jnp.logical_and(px == 1, pz == 0))
    relay = jnp.logical_or(by_z, by_x)
    relay_out = jnp.logical_and(upper, relay)
    back_z, back_x = jnp.logical_and(py == 0, by_z), jnp.logical_and(py == 0, by_x)
    turned, thick = pl.ds(*spans[early - 1]), via.shape[1]
    over_z, over_x, straight = pl.ds(0, thick), pl.ds(thick, thick), pl.ds(2 * thick, cx - 2 * thick)

    def hop(src, dst, send_sem, recv_sem, peer):
        return pltpu.make_async_remote_copy(
            src_ref=src, dst_ref=dst, send_sem=send_sem, recv_sem=recv_sem, device_id=peer, device_id_type=MESH)

    if relayed:
        across_y = (px, y_right, pz)
        direct = hop(fields.at[turned, straight], ys.at[0, turned, straight], y_send.at[0], y_recv.at[0, early - 1], across_y)
        out_z = hop(u.at[turned, over_z], via, y_send.at[0], via_recv, to_right)
        out_x = hop(u.at[turned, over_x], via, y_send.at[0], via_recv, right_x)
        over = hop(via, via, sent, via_recv, across_y)
        home_z = hop(via, ys.at[0, turned, over_z], sent, y_recv.at[0, early - 1], to_left)
        home_x = hop(via, ys.at[0, turned, over_x], sent, y_recv.at[0, early - 1], left_x)

    def settle(ref, semaphore):
        pltpu.make_async_copy(ref, ref, semaphore).wait()

    def start_y(rows):
        for row in rows:
            for copy in row:
                copy.start()

    def early_sent():
        for side in range(len(y_peers)):
            settle(u.at[pl.ds(0, mark)], y_send.at[side])

    greeters = (pz > 0).astype(jnp.int32) + (2 * (1 - lax.rem(px, 2)) if paired else 2)
    pl.semaphore_wait(barrier, len(y_peers) + greeters)
    def start_early():
        if relayed:
            start_y(y_copies[:early - 1])
            pl.when(source)(direct.start)
            pl.when(jnp.logical_not(source))(lambda: start_y(y_copies[early - 1:early]))
        else:
            start_y(y_copies[:early])

    unloaded = lax.rem(py, 2) == 1
    pl.when(unloaded)(start_early)
    load.wait()
    pl.when(jnp.logical_not(unloaded))(lambda: start_y(loaded_copies))
    gains.start()
    if held:
        at_once = jnp.logical_not(jnp.logical_or(odd, relay_out) if relayed else odd)
        pl.when(at_once)(lambda: start_y(y_copies[early:]))
    if paired:
        pl.when(jnp.logical_not(odd))(lambda: both_x(answers.at[0]))
    pl.when(pz > 0)(lambda: tell(answers.at[1], to_left))
    pl.when(last_z)(lambda: tell(answers.at[2], to_left))
    if paired:
        pl.when(odd)(lambda: pl.semaphore_wait(answers.at[0], 2))
    if relayed:
        pl.when(source)(out_x.start)
    for copy in x_copies:
        copy.start()

    lane = lax.broadcasted_iota(jnp.int32, (cx, cy, cz), 2)
    slot = lane // SLOT
    for p in range(rows_packed):
        first = p * groups
        here = min(groups, species - first)

        def pack(g, carry):
            head, tail = carry
            v = u[first + g]
            mine = slot == g
            head = jnp.where(mine, pltpu.roll(v, g * SLOT, 2), head)
            tail = jnp.where(mine, pltpu.roll(v, lax.rem((g + 1) * SLOT, cz), 2), tail)
            return head, tail

        zero = jnp.zeros((cx, cy, cz), jnp.float32)
        head, tail = each(0, here, AT_ONCE[0], pack, (zero, zero))
        packed[0, p] = head
        packed[1, p] = tail

    z_copies = [
        pltpu.make_async_remote_copy(
            src_ref=packed.at[side], dst_ref=landed.at[side],
            send_sem=sent, recv_sem=z_recv,
            device_id=(px, py, peer), device_id_type=MESH)
        for side, peer in enumerate((z_left, z_right))
    ]

    gains.wait()

    def start_right():
        pl.semaphore_wait(answers.at[1], 1)
        z_copies[1].start()

    def pass_token():
        pl.semaphore_wait(answers.at[2], 1)
        tell(answers.at[2], to_left)

    def close_ring():
        pl.semaphore_wait(answers.at[2], 1)
        tell(answers.at[1], to_left)
        z_copies[0].start()

    def end_ring():
        pl.semaphore_wait(answers.at[1], 1)
        z_copies[1].start()

    def forward(hop):
        settle(via, via_recv)
        hop.start()

    pl.when(pz < nz - 1)(start_right)
    if relayed:
        pl.when(source)(out_z.start)
    pl.when(pz > 0)(z_copies[0].start)
    pl.when(jnp.logical_and(pz > 0, pz < nz - 1))(pass_token)
    pl.when(first_z)(close_ring)

    own = [row_weights(cy, cz, r, (0,)) for r in range(cy)]
    if ny == 2:
        remote = [[row_weights(cy, cz, r, (cy, -cy)) for r in range(cy)]]
    else:
        remote = [[row_weights(cy, cz, r, (base,)) for r in range(cy)] for base in (-cy, cy)]
    inside = lane_weights(cz, (0,), 2.0 * WEIGHTS[0])
    across = lane_weights(cz, (cz, -cz), WEIGHTS[0])

    def along_own(s, _):
        v = u[s]
        total = along_lanes(v.reshape(cx * cy, cz), inside).reshape(cx, cy, cz)
        acc[s] = total + rows_sum(v, own)
        return 0

    each(0, species, AT_ONCE[1], along_own)
    pl.when(last_z)(end_ring)
    settle(landed, z_recv)

    def along_z(s, _):
        p, g = s // groups, lax.rem(s, groups)
        after = pltpu.roll(landed[0, p], lax.rem(cz - g * SLOT, cz), 2)
        before = pltpu.roll(landed[1, p], cz - (g + 1) * SLOT, 2)
        halo = jnp.where(lane < cz // 2, after, before)
        acc[s] = acc[s] + along_lanes(halo.reshape(cx * cy, cz), across).reshape(cx, cy, cz)
        return 0

    each(0, species, AT_ONCE[2], along_z)
    if relayed:
        def forward_out():
            forward(over)
            pl.when(jnp.logical_not(odd))(lambda: start_y(y_copies[early:]))

        pl.when(relay_out)(forward_out)

    def along_x(s, _):
        cells = [xs[0, s, i] for i in range(REACH)] + [u[s, i] for i in range(cx)]
        cells += [xs[1, s, i] for i in range(REACH)]
        for i in range(cx):
            total = acc[s, i]
            for d in range(1, REACH + 1):
                total = total + WEIGHTS[d] * (cells[REACH + i - d] + cells[REACH + i + d])
            acc[s, i] = total
        return 0

    def along_y(s, _):
        total = acc[s]
        for side, weights in enumerate(remote):
            total = total + rows_sum(ys[side, s], weights)
        out[s] = u[s] + (strength[s] * (1.0 / 1024.0)) * total
        return 0

    def go_on():
        pl.semaphore_wait(turn, 1)
        start_y(y_copies[early:])

    def pass_on():
        early_sent()
        tell(turn, right_x)

    if held:
        pl.when(jnp.logical_not(odd))(pass_on)
    if relayed:
        pl.when(back_x)(lambda: forward(home_x))
    settle(xs, x_recv)
    lax.fori_loop(0, species, along_x, 0)
    if held:
        pl.when(odd)(go_on)
    if relayed:
        pl.when(back_z)(lambda: forward(home_z))
    for k, (begin, size) in enumerate(spans):
        for side in range(len(y_peers)):
            settle(ys.at[side, pl.ds(begin, size)], y_recv.at[side, k])
        lax.fori_loop(begin, begin + size, along_y, 0)
    if held:
        pl.when(odd)(early_sent)
    else:
        early_sent()
    layers = 2 * species * REACH + 2 * rows_packed * cx + len(y_peers) * (species - mark) * cx
    if relayed:
        pl.when(relay)(lambda: settle(tiles.at[pl.ds(0, layers + via.shape[0] * thick)], sent))
        pl.when(jnp.logical_not(relay))(lambda: settle(tiles.at[pl.ds(0, layers)], sent))
    else:
        settle(tiles.at[pl.ds(0, layers)], sent)


def write(filtered, out, done):
    for s in range(filtered.shape[0]):
        pltpu.make_async_copy(filtered.at[s], out.at[s], done).start()
    pltpu.make_async_copy(filtered, out, done).wait()


def local(nx, ny, nz, fields, strength):
    species, cx, cy, cz = fields.shape
    cuts = CUTS if sum(CUTS) == species else (1,) * species
    pieces = len(cuts)
    early = EARLY if sum(CUTS) == species and nx % 2 == 0 else pieces
    sides = 1 if ny == 2 else 2
    groups = cz // SLOT
    rows_packed = -(-species // groups)
    block = (species, cx, cy, cz)
    layers = 2 * species * REACH + 2 * rows_packed * cx + sides * species * cx + species * DETOUR
    dma = pltpu.SemaphoreType.DMA
    filtered = pl.pallas_call(
        functools.partial(kernel, nx, ny, nz, cuts, early),
        out_shape=pltpu.VMEM(block, jnp.float32),
        in_specs=[pl.BlockSpec(memory_space=pltpu.HBM), pl.BlockSpec(memory_space=pl.ANY)],
        out_specs=pl.BlockSpec(memory_space=pltpu.VMEM),
        scratch_shapes=[
            pltpu.SMEM((species,), jnp.float32),
            pltpu.VMEM(block, jnp.float32),
            pltpu.VMEM(block, jnp.float32),
            pltpu.VMEM((layers, cy, cz), jnp.float32),
            pltpu.VMEM((2, species, REACH, cy, cz), jnp.float32),
            pltpu.VMEM((sides,) + block, jnp.float32),
            pltpu.VMEM((2, rows_packed, cx, cy, cz), jnp.float32),
            pltpu.VMEM((2, rows_packed, cx, cy, cz), jnp.float32),
            pltpu.VMEM((cuts[early - 1], DETOUR, cy, cz), jnp.float32),
            dma,
            dma,
            dma,
            dma((sides,)),
            dma((sides, pieces)),
            dma,
            dma,
            pltpu.SemaphoreType.REGULAR((3,)),
            pltpu.SemaphoreType.REGULAR,
        ],
        compiler_params=pltpu.CompilerParams(collective_id=0, has_side_effects=True, vmem_limit_bytes=56 * 1024 * 1024),
        name="filter_pass",
    )(fields, strength)
    return pl.pallas_call(
        write,
        out_shape=pltpu.HBM(block, jnp.float32),
        in_specs=[pl.BlockSpec(memory_space=pltpu.VMEM)],
        out_specs=pl.BlockSpec(memory_space=pltpu.HBM),
        scratch_shapes=[dma],
        compiler_params=pltpu.CompilerParams(vmem_limit_bytes=4 * 1024 * 1024),
        name="write",
    )(filtered)


def solution(mesh):
    sizes = mesh.shape
    return jax.shard_map(
        functools.partial(local, sizes["gx"], sizes["gy"], sizes["gz"]),
        mesh=mesh,
        in_specs=(P(None, "gx", "gy", "gz"), P()),
        out_specs=P(None, "gx", "gy", "gz"),
        check_vma=False,
    )
```

```python
import functools
import jax
import jax.numpy as jnp
from jax import lax
from jax.experimental import pallas as pl
from jax.experimental.pallas import tpu as pltpu
from jax.sharding import PartitionSpec as P

MESH = pl.DeviceIdType.MESH
REACH = 5
SLOT = 8
WEIGHTS = [-252.0, 210.0, -120.0, 45.0, -10.0, 1.0]
CUTS = (19, 5, 6, 2)
EARLY = 2
DETOUR = 1
AT_ONCE = (8, 4, 8)


def each(begin, count, at_once, body, carry=0):
    step = at_once if count % at_once == 0 else 1

    def steps(k, carry):
        for i in range(step):
            carry = body(begin + k * step + i, carry)
        return carry

    return lax.fori_loop(0, count // step, steps, carry)


def weight_of(offset):
    return WEIGHTS[abs(offset)] if abs(offset) <= REACH else 0.0


def row_weights(rows, lanes, roll, bases):
    row = lax.broadcasted_iota(jnp.int32, (rows, lanes), 0)
    out = jnp.zeros((rows, lanes), jnp.float32)
    for i in range(rows):
        value = sum(weight_of((i + roll) % rows + base - i) for base in bases)
        if value:
            out = jnp.where(row == i, value, out)
    return out


def lane_weights(lanes, bases, centre):
    source = lax.broadcasted_iota(jnp.int32, (lanes, lanes), 0)
    offset = source - lax.broadcasted_iota(jnp.int32, (lanes, lanes), 1)
    out = jnp.zeros((lanes, lanes), jnp.float32)
    for base in bases:
        for d in range(-REACH, REACH + 1):
            out = jnp.where(offset + base == d, centre if d == 0 else weight_of(d), out)
    return out.astype(jnp.bfloat16)


def along_lanes(rows, weights):
    total = None
    for part in range(3):
        piece = rows.astype(jnp.bfloat16)
        rows = rows - piece.astype(jnp.float32)
        term = jnp.dot(piece, weights, preferred_element_type=jnp.float32)
        total = term if total is None else total + term
    return total


def rolled_rows(block, roll):
    rows = block.shape[1]
    return block if roll == 0 else pltpu.roll(block, rows - roll, 1)


def rows_sum(block, weights):
    total = None
    for roll, weight in enumerate(weights):
        term = weight[None] * rolled_rows(block, roll)
        total = term if total is None else total + term
    return total


def kernel(nx, ny, nz, cuts, early, fields, strength_in, out, strength, u, acc, tiles, xs, ys, packed, landed, via,
           in_sem, sent, x_recv, y_send, y_recv, z_recv, via_recv, answers, turn):
    species, cx, cy, cz = u.shape
    groups = cz // SLOT
    rows_packed = packed.shape[1]
    px, py, pz = lax.axis_index("gx"), lax.axis_index("gy"), lax.axis_index("gz")
    x_left, x_right = lax.rem(px + nx - 1, nx), lax.rem(px + 1, nx)
    y_left, y_right = lax.rem(py + ny - 1, ny), lax.rem(py + 1, ny)
    z_left, z_right = lax.rem(pz + nz - 1, nz), lax.rem(pz + 1, nz)
    y_peers = [y_right] if ny == 2 else [y_right, y_left]

    barrier = pltpu.get_barrier_semaphore()
    to_left, to_right = (px, py, z_left), (px, py, z_right)
    left_x, right_x = (x_left, py, pz), (x_right, py, pz)
    first_z, last_z = pz == 0, pz == nz - 1

    def tell(semaphore, peer):
        pl.semaphore_signal(semaphore, inc=1, device_id=peer, device_id_type=MESH)

    for peer in y_peers:
        tell(barrier, (px, peer, pz))
    odd = lax.rem(px, 2) == 1
    paired = nx % 2 == 0

    def both_x(semaphore):
        tell(semaphore, left_x)
        tell(semaphore, right_x)

    if paired:
        pl.when(odd)(lambda: both_x(barrier))
    else:
        both_x(barrier)
    pl.when(pz < nz - 1)(lambda: tell(barrier, to_right))

    spans = []
    begin = 0
    for size in cuts:
        spans.append((begin, size))
        begin += size
    load = pltpu.make_async_copy(fields, u, in_sem)
    gains = pltpu.make_async_copy(strength_in, strength, in_sem)
    load.start()

    held = early < len(cuts)
    mark = sum(cuts[:early])

    def y_row(k, source):
        part = pl.ds(*spans[k])
        return [
            pltpu.make_async_remote_copy(
                src_ref=source.at[part], dst_ref=ys.at[side, part],
                send_sem=y_send.at[side] if k < early else sent, recv_sem=y_recv.at[side, k],
                device_id=(px, peer, pz), device_id_type=MESH)
            for side, peer in enumerate(y_peers)]

    y_copies = [y_row(k, fields if k < early else u) for k in range(len(spans))]
    loaded_copies = [y_row(k, u) for k in range(early)]
    x_copies = [
        pltpu.make_async_remote_copy(
            src_ref=u.at[:, pl.ds(begin, REACH)], dst_ref=xs.at[side],
            send_sem=sent, recv_sem=x_recv,
            device_id=(peer, py, pz), device_id_type=MESH)
        for side, (begin, peer) in enumerate(((cx - REACH, x_right), (0, x_left)))
    ]

    relayed = held and ny == 2 and nz > 1 and nx > 2 and cx > 2 * via.shape[1]
    by_z, by_x = jnp.logical_and(px == 1, pz == 1), jnp.logical_and(px == 2, pz == 0)
    upper = py == 1
    source = jnp.logical_and(upper, jnp.logical_and(px == 1, pz == 0))
    relay = jnp.logical_or(by_z, by_x)
    relay_out = jnp.logical_and(upper, relay)
    back_z, back_x = jnp.logical_and(py == 0, by_z), jnp.logical_and(py == 0, by_x)
    turned, thick = pl.ds(*spans[early - 1]), via.shape[1]
    over_z, over_x, straight = pl.ds(0, thick), pl.ds(thick, thick), pl.ds(2 * thick, cx - 2 * thick)

    def hop(src, dst, send_sem, recv_sem, peer):
        return pltpu.make_async_remote_copy(
            src_ref=src, dst_ref=dst, send_sem=send_sem, recv_sem=recv_sem, device_id=peer, device_id_type=MESH)

    if relayed:
        across_y = (px, y_right, pz)
        direct = hop(fields.at[turned, straight], ys.at[0, turned, straight], y_send.at[0], y_recv.at[0, early - 1], across_y)
        out_z = hop(u.at[turned, over_z], via, y_send.at[0], via_recv, to_right)
        out_x = hop(u.at[turned, over_x], via, y_send.at[0], via_recv, right_x)
        over = hop(via, via, sent, via_recv, across_y)
        home_z = hop(via, ys.at[0, turned, over_z], sent, y_recv.at[0, early - 1], to_left)
        home_x = hop(via, ys.at[0, turned, over_x], sent, y_recv.at[0, early - 1], left_x)

    def settle(ref, semaphore):
        pltpu.make_async_copy(ref, ref, semaphore).wait()

    def start_y(rows):
        for row in rows:
            for copy in row:
                copy.start()

    def early_sent():
        for side in range(len(y_peers)):
            settle(u.at[pl.ds(0, mark)], y_send.at[side])

    greeters = (pz > 0).astype(jnp.int32) + (2 * (1 - lax.rem(px, 2)) if paired else 2)
    pl.semaphore_wait(barrier, len(y_peers) + greeters)
    def start_early():
        if relayed:
            start_y(y_copies[:early - 1])
            pl.when(source)(direct.start)
            pl.when(jnp.logical_not(source))(lambda: start_y(y_copies[early - 1:early]))
        else:
            start_y(y_copies[:early])

    unloaded = lax.rem(py, 2) == 1
    pl.when(unloaded)(start_early)
    load.wait()
    pl.when(jnp.logical_not(unloaded))(lambda: start_y(loaded_copies))
    gains.start()
    if held:
        at_once = jnp.logical_not(jnp.logical_or(odd, relay_out) if relayed else odd)
        pl.when(at_once)(lambda: start_y(y_copies[early:]))
    if paired:
        pl.when(jnp.logical_not(odd))(lambda: both_x(answers.at[0]))
    pl.when(pz > 0)(lambda: tell(answers.at[1], to_left))
    pl.when(last_z)(lambda: tell(answers.at[2], to_left))
    if paired:
        pl.when(odd)(lambda: pl.semaphore_wait(answers.at[0], 2))
    if relayed:
        pl.when(source)(out_x.start)
    for copy in x_copies:
        copy.start()

    lane = lax.broadcasted_iota(jnp.int32, (cx, cy, cz), 2)
    slot = lane // SLOT
    for p in range(rows_packed):
        first = p * groups
        here = min(groups, species - first)

        def pack(g, carry):
            head, tail = carry
            v = u[first + g]
            mine = slot == g
            head = jnp.where(mine, pltpu.roll(v, g * SLOT, 2), head)
            tail = jnp.where(mine, pltpu.roll(v, lax.rem((g + 1) * SLOT, cz), 2), tail)
            return head, tail

        zero = jnp.zeros((cx, cy, cz), jnp.float32)
        head, tail = each(0, here, AT_ONCE[0], pack, (zero, zero))
        packed[0, p] = head
        packed[1, p] = tail

    z_copies = [
        pltpu.make_async_remote_copy(
            src_ref=packed.at[side], dst_ref=landed.at[side],
            send_sem=sent, recv_sem=z_recv,
            device_id=(px, py, peer), device_id_type=MESH)
        for side, peer in enumerate((z_left, z_right))
    ]

    gains.wait()

    def start_right():
        pl.semaphore_wait(answers.at[1], 1)
        z_copies[1].start()

    def pass_token():
        pl.semaphore_wait(answers.at[2], 1)
        tell(answers.at[2], to_left)

    def close_ring():
        pl.semaphore_wait(answers.at[2], 1)
        tell(answers.at[1], to_left)
        z_copies[0].start()

    def end_ring():
        pl.semaphore_wait(answers.at[1], 1)
        z_copies[1].start()

    def forward(hop):
        settle(via, via_recv)
        hop.start()

    pl.when(pz < nz - 1)(start_right)
    if relayed:
        pl.when(source)(out_z.start)
    pl.when(pz > 0)(z_copies[0].start)
    pl.when(jnp.logical_and(pz > 0, pz < nz - 1))(pass_token)
    pl.when(first_z)(close_ring)

    own = [row_weights(cy, cz, r, (0,)) for r in range(cy)]
    if ny == 2:
        remote = [[row_weights(cy, cz, r, (cy, -cy)) for r in range(cy)]]
    else:
        remote = [[row_weights(cy, cz, r, (base,)) for r in range(cy)] for base in (-cy, cy)]
    inside = lane_weights(cz, (0,), 2.0 * WEIGHTS[0])
    across = lane_weights(cz, (cz, -cz), WEIGHTS[0])

    def along_own(s, _):
        v = u[s]
        total = along_lanes(v.reshape(cx * cy, cz), inside).reshape(cx, cy, cz)
        acc[s] = total + rows_sum(v, own)
        return 0

    each(0, species, AT_ONCE[1], along_own)
    pl.when(last_z)(end_ring)
    settle(landed, z_recv)

    def along_z(s, _):
        p, g = s // groups, lax.rem(s, groups)
        after = pltpu.roll(landed[0, p], lax.rem(cz - g * SLOT, cz), 2)
        before = pltpu.roll(landed[1, p], cz - (g + 1) * SLOT, 2)
        halo = jnp.where(lane < cz // 2, after, before)
        acc[s] = acc[s] + along_lanes(halo.reshape(cx * cy, cz), across).reshape(cx, cy, cz)
        return 0

    each(0, species, AT_ONCE[2], along_z)
    if relayed:
        def forward_out():
            forward(over)
            pl.when(jnp.logical_not(odd))(lambda: start_y(y_copies[early:]))

        pl.when(relay_out)(forward_out)

    def along_x(s, _):
        cells = [xs[0, s, i] for i in range(REACH)] + [u[s, i] for i in range(cx)]
        cells += [xs[1, s, i] for i in range(REACH)]
        for i in range(cx):
            total = acc[s, i]
            for d in range(1, REACH + 1):
                total = total + WEIGHTS[d] * (cells[REACH + i - d] + cells[REACH + i + d])
            acc[s, i] = total
        return 0

    def along_y(s, _):
        total = acc[s]
        for side, weights in enumerate(remote):
            total = total + rows_sum(ys[side, s], weights)
        out[s] = u[s] + (strength[s] * (1.0 / 1024.0)) * total
        return 0

    def go_on():
        pl.semaphore_wait(turn, 1)
        start_y(y_copies[early:])

    def pass_on():
        early_sent()
        tell(turn, right_x)

    if held:
        pl.when(jnp.logical_not(odd))(pass_on)
    if relayed:
        pl.when(back_x)(lambda: forward(home_x))
    settle(xs, x_recv)
    lax.fori_loop(0, species, along_x, 0)
    if held:
        pl.when(odd)(go_on)
    if relayed:
        pl.when(back_z)(lambda: forward(home_z))
    for k, (begin, size) in enumerate(spans):
        for side in range(len(y_peers)):
            settle(ys.at[side, pl.ds(begin, size)], y_recv.at[side, k])
        lax.fori_loop(begin, begin + size, along_y, 0)
    if held:
        pl.when(odd)(early_sent)
    else:
        early_sent()
    layers = 2 * species * REACH + 2 * rows_packed * cx + len(y_peers) * (species - mark) * cx
    if relayed:
        pl.when(relay)(lambda: settle(tiles.at[pl.ds(0, layers + via.shape[0] * thick)], sent))
        pl.when(jnp.logical_not(relay))(lambda: settle(tiles.at[pl.ds(0, layers)], sent))
    else:
        settle(tiles.at[pl.ds(0, layers)], sent)


def write(filtered, out, done):
    for s in range(filtered.shape[0]):
        pltpu.make_async_copy(filtered.at[s], out.at[s], done).start()
    pltpu.make_async_copy(filtered, out, done).wait()


def local(nx, ny, nz, fields, strength):
    species, cx, cy, cz = fields.shape
    cuts = CUTS if sum(CUTS) == species else (1,) * species
    pieces = len(cuts)
    early = EARLY if sum(CUTS) == species and nx % 2 == 0 else pieces
    sides = 1 if ny == 2 else 2
    groups = cz // SLOT
    rows_packed = -(-species // groups)
    block = (species, cx, cy, cz)
    layers = 2 * species * REACH + 2 * rows_packed * cx + sides * species * cx + species * DETOUR
    dma = pltpu.SemaphoreType.DMA
    filtered = pl.pallas_call(
        functools.partial(kernel, nx, ny, nz, cuts, early),
        out_shape=pltpu.VMEM(block, jnp.float32),
        in_specs=[pl.BlockSpec(memory_space=pltpu.HBM), pl.BlockSpec(memory_space=pl.ANY)],
        out_specs=pl.BlockSpec(memory_space=pltpu.VMEM),
        scratch_shapes=[
            pltpu.SMEM((species,), jnp.float32),
            pltpu.VMEM(block, jnp.float32),
            pltpu.VMEM(block, jnp.float32),
            pltpu.VMEM((layers, cy, cz), jnp.float32),
            pltpu.VMEM((2, species, REACH, cy, cz), jnp.float32),
            pltpu.VMEM((sides,) + block, jnp.float32),
            pltpu.VMEM((2, rows_packed, cx, cy, cz), jnp.float32),
            pltpu.VMEM((2, rows_packed, cx, cy, cz), jnp.float32),
            pltpu.VMEM((cuts[early - 1], DETOUR, cy, cz), jnp.float32),
            dma,
            dma,
            dma,
            dma((sides,)),
            dma((sides, pieces)),
            dma,
            dma,
            pltpu.SemaphoreType.REGULAR((3,)),
            pltpu.SemaphoreType.REGULAR,
        ],
        compiler_params=pltpu.CompilerParams(collective_id=0, has_side_effects=True, vmem_limit_bytes=56 * 1024 * 1024),
        name="filter_pass",
    )(fields, strength)
    return pl.pallas_call(
        write,
        out_shape=pltpu.HBM(block, jnp.float32),
        in_specs=[pl.BlockSpec(memory_space=pltpu.VMEM)],
        out_specs=pl.BlockSpec(memory_space=pltpu.HBM),
        scratch_shapes=[dma],
        compiler_params=pltpu.CompilerParams(vmem_limit_bytes=4 * 1024 * 1024),
        name="write",
    )(filtered)


def solution(mesh):
    sizes = mesh.shape
    return jax.shard_map(
        functools.partial(local, sizes["gx"], sizes["gy"], sizes["gz"]),
        mesh=mesh,
        in_specs=(P(None, "gx", "gy", "gz"), P()),
        out_specs=P(None, "gx", "gy", "gz"),
        check_vma=False,
    )
```

```python
import functools
import jax
import jax.numpy as jnp
from jax import lax
from jax.experimental import pallas as pl
from jax.experimental.pallas import tpu as pltpu
from jax.sharding import PartitionSpec as P

MESH = pl.DeviceIdType.MESH
REACH = 5
SLOT = 8
WEIGHTS = [-252.0, 210.0, -120.0, 45.0, -10.0, 1.0]
CUTS = (19, 5, 7, 1)
EARLY = 2
DETOUR = 1
AT_ONCE = (8, 4, 8)


def each(begin, count, at_once, body, carry=0):
    step = at_once if count % at_once == 0 else 1

    def steps(k, carry):
        for i in range(step):
            carry = body(begin + k * step + i, carry)
        return carry

    return lax.fori_loop(0, count // step, steps, carry)


def weight_of(offset):
    return WEIGHTS[abs(offset)] if abs(offset) <= REACH else 0.0


def row_weights(rows, lanes, roll, bases):
    row = lax.broadcasted_iota(jnp.int32, (rows, lanes), 0)
    out = jnp.zeros((rows, lanes), jnp.float32)
    for i in range(rows):
        value = sum(weight_of((i + roll) % rows + base - i) for base in bases)
        if value:
            out = jnp.where(row == i, value, out)
    return out


def lane_weights(lanes, bases, centre):
    source = lax.broadcasted_iota(jnp.int32, (lanes, lanes), 0)
    offset = source - lax.broadcasted_iota(jnp.int32, (lanes, lanes), 1)
    out = jnp.zeros((lanes, lanes), jnp.float32)
    for base in bases:
        for d in range(-REACH, REACH + 1):
            out = jnp.where(offset + base == d, centre if d == 0 else weight_of(d), out)
    return out.astype(jnp.bfloat16)


def along_lanes(rows, weights):
    total = None
    for part in range(3):
        piece = rows.astype(jnp.bfloat16)
        rows = rows - piece.astype(jnp.float32)
        term = jnp.dot(piece, weights, preferred_element_type=jnp.float32)
        total = term if total is None else total + term
    return total


def rolled_rows(block, roll):
    rows = block.shape[1]
    return block if roll == 0 else pltpu.roll(block, rows - roll, 1)


def rows_sum(block, weights):
    total = None
    for roll, weight in enumerate(weights):
        term = weight[None] * rolled_rows(block, roll)
        total = term if total is None else total + term
    return total


def kernel(nx, ny, nz, cuts, early, fields, strength_in, out, strength, u, acc, tiles, xs, ys, packed, landed, via,
           in_sem, sent, x_recv, y_send, y_recv, z_recv, via_recv, answers, turn):
    species, cx, cy, cz = u.shape
    groups = cz // SLOT
    rows_packed = packed.shape[1]
    px, py, pz = lax.axis_index("gx"), lax.axis_index("gy"), lax.axis_index("gz")
    x_left, x_right = lax.rem(px + nx - 1, nx), lax.rem(px + 1, nx)
    y_left, y_right = lax.rem(py + ny - 1, ny), lax.rem(py + 1, ny)
    z_left, z_right = lax.rem(pz + nz - 1, nz), lax.rem(pz + 1, nz)
    y_peers = [y_right] if ny == 2 else [y_right, y_left]

    barrier = pltpu.get_barrier_semaphore()
    to_left, to_right = (px, py, z_left), (px, py, z_right)
    left_x, right_x = (x_left, py, pz), (x_right, py, pz)
    first_z, last_z = pz == 0, pz == nz - 1

    def tell(semaphore, peer):
        pl.semaphore_signal(semaphore, inc=1, device_id=peer, device_id_type=MESH)

    for peer in y_peers:
        tell(barrier, (px, peer, pz))
    odd = lax.rem(px, 2) == 1
    paired = nx % 2 == 0

    def both_x(semaphore):
        tell(semaphore, left_x)
        tell(semaphore, right_x)

    if paired:
        pl.when(odd)(lambda: both_x(barrier))
    else:
        both_x(barrier)
    pl.when(pz < nz - 1)(lambda: tell(barrier, to_right))

    spans = []
    begin = 0
    for size in cuts:
        spans.append((begin, size))
        begin += size
    load = pltpu.make_async_copy(fields, u, in_sem)
    gains = pltpu.make_async_copy(strength_in, strength, in_sem)
    unloaded = lax.rem(py, 2) == 1
    pl.when(jnp.logical_not(unloaded))(load.start)

    held = early < len(cuts)
    mark = sum(cuts[:early])

    def y_row(k, source):
        part = pl.ds(*spans[k])
        return [
            pltpu.make_async_remote_copy(
                src_ref=source.at[part], dst_ref=ys.at[side, part],
                send_sem=y_send.at[side] if k < early else sent, recv_sem=y_recv.at[side, k],
                device_id=(px, peer, pz), device_id_type=MESH)
            for side, peer in enumerate(y_peers)]

    y_copies = [y_row(k, fields if k < early else u) for k in range(len(spans))]
    loaded_copies = [y_row(k, u) for k in range(early)]
    x_copies = [
        pltpu.make_async_remote_copy(
            src_ref=u.at[:, pl.ds(begin, REACH)], dst_ref=xs.at[side],
            send_sem=sent, recv_sem=x_recv,
            device_id=(peer, py, pz), device_id_type=MESH)
        for side, (begin, peer) in enumerate(((cx - REACH, x_right), (0, x_left)))
    ]

    relayed = held and ny == 2 and nz > 1 and nx > 2 and cx > 2 * via.shape[1]
    by_z, by_x = jnp.logical_and(px == 1, pz == 1), jnp.logical_and(px == 2, pz == 0)
    upper = py == 1
    source = jnp.logical_and(upper, jnp.logical_and(px == 1, pz == 0))
    relay = jnp.logical_or(by_z, by_x)
    relay_out = jnp.logical_and(upper, relay)
    back_z, back_x = jnp.logical_and(py == 0, by_z), jnp.logical_and(py == 0, by_x)
    turned, thick = pl.ds(*spans[early - 1]), via.shape[1]
    over_z, over_x, straight = pl.ds(0, thick), pl.ds(thick, thick), pl.ds(2 * thick, cx - 2 * thick)

    def hop(src, dst, send_sem, recv_sem, peer):
        return pltpu.make_async_remote_copy(
            src_ref=src, dst_ref=dst, send_sem=send_sem, recv_sem=recv_sem, device_id=peer, device_id_type=MESH)

    if relayed:
        across_y = (px, y_right, pz)
        direct = hop(fields.at[turned, straight], ys.at[0, turned, straight], y_send.at[0], y_recv.at[0, early - 1], across_y)
        out_z = hop(u.at[turned, over_z], via, y_send.at[0], via_recv, to_right)
        out_x = hop(u.at[turned, over_x], via, y_send.at[0], via_recv, right_x)
        over = hop(via, via, sent, via_recv, across_y)
        home_z = hop(via, ys.at[0, turned, over_z], sent, y_recv.at[0, early - 1], to_left)
        home_x = hop(via, ys.at[0, turned, over_x], sent, y_recv.at[0, early - 1], left_x)

    def settle(ref, semaphore):
        pltpu.make_async_copy(ref, ref, semaphore).wait()

    def start_y(rows):
        for row in rows:
            for copy in row:
                copy.start()

    def early_sent():
        for side in range(len(y_peers)):
            settle(u.at[pl.ds(0, mark)], y_send.at[side])

    greeters = (pz > 0).astype(jnp.int32) + (2 * (1 - lax.rem(px, 2)) if paired else 2)
    pl.semaphore_wait(barrier, len(y_peers) + greeters)
    def start_early():
        if relayed:
            start_y(y_copies[:early - 1])
            pl.when(source)(direct.start)
            pl.when(jnp.logical_not(source))(lambda: start_y(y_copies[early - 1:early]))
        else:
            start_y(y_copies[:early])

    pl.when(unloaded)(start_early)
    pl.when(unloaded)(load.start)
    load.wait()
    pl.when(jnp.logical_not(unloaded))(lambda: start_y(loaded_copies))
    gains.start()
    if held:
        at_once = jnp.logical_not(jnp.logical_or(odd, relay_out) if relayed else odd)
        pl.when(at_once)(lambda: start_y(y_copies[early:]))
    if paired:
        pl.when(jnp.logical_not(odd))(lambda: both_x(answers.at[0]))
    pl.when(pz > 0)(lambda: tell(answers.at[1], to_left))
    pl.when(last_z)(lambda: tell(answers.at[2], to_left))
    if paired:
        pl.when(odd)(lambda: pl.semaphore_wait(answers.at[0], 2))
    if relayed:
        pl.when(source)(out_x.start)
    for copy in x_copies:
        copy.start()

    lane = lax.broadcasted_iota(jnp.int32, (cx, cy, cz), 2)
    slot = lane // SLOT
    for p in range(rows_packed):
        first = p * groups
        here = min(groups, species - first)

        def pack(g, carry):
            head, tail = carry
            v = u[first + g]
            mine = slot == g
            head = jnp.where(mine, pltpu.roll(v, g * SLOT, 2), head)
            tail = jnp.where(mine, pltpu.roll(v, lax.rem((g + 1) * SLOT, cz), 2), tail)
            return head, tail

        zero = jnp.zeros((cx, cy, cz), jnp.float32)
        head, tail = each(0, here, AT_ONCE[0], pack, (zero, zero))
        packed[0, p] = head
        packed[1, p] = tail

    z_copies = [
        pltpu.make_async_remote_copy(
            src_ref=packed.at[side], dst_ref=landed.at[side],
            send_sem=sent, recv_sem=z_recv,
            device_id=(px, py, peer), device_id_type=MESH)
        for side, peer in enumerate((z_left, z_right))
    ]

    gains.wait()

    def start_right():
        pl.semaphore_wait(answers.at[1], 1)
        z_copies[1].start()

    def pass_token():
        pl.semaphore_wait(answers.at[2], 1)
        tell(answers.at[2], to_left)

    def close_ring():
        pl.semaphore_wait(answers.at[2], 1)
        tell(answers.at[1], to_left)
        z_copies[0].start()

    def end_ring():
        pl.semaphore_wait(answers.at[1], 1)
        z_copies[1].start()

    def forward(hop):
        settle(via, via_recv)
        hop.start()

    pl.when(pz < nz - 1)(start_right)
    if relayed:
        pl.when(source)(out_z.start)
    pl.when(pz > 0)(z_copies[0].start)
    pl.when(jnp.logical_and(pz > 0, pz < nz - 1))(pass_token)
    pl.when(first_z)(close_ring)

    own = [row_weights(cy, cz, r, (0,)) for r in range(cy)]
    if ny == 2:
        remote = [[row_weights(cy, cz, r, (cy, -cy)) for r in range(cy)]]
    else:
        remote = [[row_weights(cy, cz, r, (base,)) for r in range(cy)] for base in (-cy, cy)]
    inside = lane_weights(cz, (0,), 2.0 * WEIGHTS[0])
    across = lane_weights(cz, (cz, -cz), WEIGHTS[0])

    def along_own(s, _):
        v = u[s]
        total = along_lanes(v.reshape(cx * cy, cz), inside).reshape(cx, cy, cz)
        acc[s] = total + rows_sum(v, own)
        return 0

    each(0, species, AT_ONCE[1], along_own)
    pl.when(last_z)(end_ring)
    settle(landed, z_recv)

    def along_z(s, _):
        p, g = s // groups, lax.rem(s, groups)
        after = pltpu.roll(landed[0, p], lax.rem(cz - g * SLOT, cz), 2)
        before = pltpu.roll(landed[1, p], cz - (g + 1) * SLOT, 2)
        halo = jnp.where(lane < cz // 2, after, before)
        acc[s] = acc[s] + along_lanes(halo.reshape(cx * cy, cz), across).reshape(cx, cy, cz)
        return 0

    each(0, species, AT_ONCE[2], along_z)
    if relayed:
        def forward_out():
            forward(over)
            pl.when(jnp.logical_not(odd))(lambda: start_y(y_copies[early:]))

        pl.when(relay_out)(forward_out)

    def along_x(s, _):
        cells = [xs[0, s, i] for i in range(REACH)] + [u[s, i] for i in range(cx)]
        cells += [xs[1, s, i] for i in range(REACH)]
        for i in range(cx):
            total = acc[s, i]
            for d in range(1, REACH + 1):
                total = total + WEIGHTS[d] * (cells[REACH + i - d] + cells[REACH + i + d])
            acc[s, i] = total
        return 0

    def along_y(s, _):
        total = acc[s]
        for side, weights in enumerate(remote):
            total = total + rows_sum(ys[side, s], weights)
        out[s] = u[s] + (strength[s] * (1.0 / 1024.0)) * total
        return 0

    def go_on():
        pl.semaphore_wait(turn, 1)
        start_y(y_copies[early:])

    def pass_on():
        early_sent()
        tell(turn, right_x)

    if held:
        pl.when(jnp.logical_not(odd))(pass_on)
    if relayed:
        pl.when(back_x)(lambda: forward(home_x))
    settle(xs, x_recv)
    lax.fori_loop(0, species, along_x, 0)
    if held:
        pl.when(odd)(go_on)
    if relayed:
        pl.when(back_z)(lambda: forward(home_z))
    for k, (begin, size) in enumerate(spans):
        for side in range(len(y_peers)):
            settle(ys.at[side, pl.ds(begin, size)], y_recv.at[side, k])
        lax.fori_loop(begin, begin + size, along_y, 0)
    if held:
        pl.when(odd)(early_sent)
    else:
        early_sent()
    layers = 2 * species * REACH + 2 * rows_packed * cx + len(y_peers) * (species - mark) * cx
    if relayed:
        pl.when(relay)(lambda: settle(tiles.at[pl.ds(0, layers + via.shape[0] * thick)], sent))
        pl.when(jnp.logical_not(relay))(lambda: settle(tiles.at[pl.ds(0, layers)], sent))
    else:
        settle(tiles.at[pl.ds(0, layers)], sent)


def write(filtered, out, done):
    for s in range(filtered.shape[0]):
        pltpu.make_async_copy(filtered.at[s], out.at[s], done).start()
    pltpu.make_async_copy(filtered, out, done).wait()


def local(nx, ny, nz, fields, strength):
    species, cx, cy, cz = fields.shape
    cuts = CUTS if sum(CUTS) == species else (1,) * species
    pieces = len(cuts)
    early = EARLY if sum(CUTS) == species and nx % 2 == 0 else pieces
    sides = 1 if ny == 2 else 2
    groups = cz // SLOT
    rows_packed = -(-species // groups)
    block = (species, cx, cy, cz)
    layers = 2 * species * REACH + 2 * rows_packed * cx + sides * species * cx + species * DETOUR
    dma = pltpu.SemaphoreType.DMA
    filtered = pl.pallas_call(
        functools.partial(kernel, nx, ny, nz, cuts, early),
        out_shape=pltpu.VMEM(block, jnp.float32),
        in_specs=[pl.BlockSpec(memory_space=pltpu.HBM), pl.BlockSpec(memory_space=pl.ANY)],
        out_specs=pl.BlockSpec(memory_space=pltpu.VMEM),
        scratch_shapes=[
            pltpu.SMEM((species,), jnp.float32),
            pltpu.VMEM(block, jnp.float32),
            pltpu.VMEM(block, jnp.float32),
            pltpu.VMEM((layers, cy, cz), jnp.float32),
            pltpu.VMEM((2, species, REACH, cy, cz), jnp.float32),
            pltpu.VMEM((sides,) + block, jnp.float32),
            pltpu.VMEM((2, rows_packed, cx, cy, cz), jnp.float32),
            pltpu.VMEM((2, rows_packed, cx, cy, cz), jnp.float32),
            pltpu.VMEM((cuts[early - 1], DETOUR, cy, cz), jnp.float32),
            dma,
            dma,
            dma,
            dma((sides,)),
            dma((sides, pieces)),
            dma,
            dma,
            pltpu.SemaphoreType.REGULAR((3,)),
            pltpu.SemaphoreType.REGULAR,
        ],
        compiler_params=pltpu.CompilerParams(collective_id=0, has_side_effects=True, vmem_limit_bytes=56 * 1024 * 1024),
        name="filter_pass",
    )(fields, strength)
    return pl.pallas_call(
        write,
        out_shape=pltpu.HBM(block, jnp.float32),
        in_specs=[pl.BlockSpec(memory_space=pltpu.VMEM)],
        out_specs=pl.BlockSpec(memory_space=pltpu.HBM),
        scratch_shapes=[dma],
        compiler_params=pltpu.CompilerParams(vmem_limit_bytes=4 * 1024 * 1024),
        name="write",
    )(filtered)


def solution(mesh):
    sizes = mesh.shape
    return jax.shard_map(
        functools.partial(local, sizes["gx"], sizes["gy"], sizes["gz"]),
        mesh=mesh,
        in_specs=(P(None, "gx", "gy", "gz"), P()),
        out_specs=P(None, "gx", "gy", "gz"),
        check_vma=False,
    )
```

```python
import functools
import jax
import jax.numpy as jnp
from jax import lax
from jax.experimental import pallas as pl
from jax.experimental.pallas import tpu as pltpu
from jax.sharding import PartitionSpec as P

MESH = pl.DeviceIdType.MESH
REACH = 5
SLOT = 8
WEIGHTS = [-252.0, 210.0, -120.0, 45.0, -10.0, 1.0]
CUTS = (18, 6, 7, 1)
EARLY = 2
DETOUR = 1
AT_ONCE = (8, 4, 8)


def each(begin, count, at_once, body, carry=0):
    step = at_once if count % at_once == 0 else 1

    def steps(k, carry):
        for i in range(step):
            carry = body(begin + k * step + i, carry)
        return carry

    return lax.fori_loop(0, count // step, steps, carry)


def weight_of(offset):
    return WEIGHTS[abs(offset)] if abs(offset) <= REACH else 0.0


def row_weights(rows, lanes, roll, bases):
    row = lax.broadcasted_iota(jnp.int32, (rows, lanes), 0)
    out = jnp.zeros((rows, lanes), jnp.float32)
    for i in range(rows):
        value = sum(weight_of((i + roll) % rows + base - i) for base in bases)
        if value:
            out = jnp.where(row == i, value, out)
    return out


def lane_weights(lanes, bases, centre):
    source = lax.broadcasted_iota(jnp.int32, (lanes, lanes), 0)
    offset = source - lax.broadcasted_iota(jnp.int32, (lanes, lanes), 1)
    out = jnp.zeros((lanes, lanes), jnp.float32)
    for base in bases:
        for d in range(-REACH, REACH + 1):
            out = jnp.where(offset + base == d, centre if d == 0 else weight_of(d), out)
    return out.astype(jnp.bfloat16)


def along_lanes(rows, weights):
    total = None
    for part in range(3):
        piece = rows.astype(jnp.bfloat16)
        rows = rows - piece.astype(jnp.float32)
        term = jnp.dot(piece, weights, preferred_element_type=jnp.float32)
        total = term if total is None else total + term
    return total


def rolled_rows(block, roll):
    rows = block.shape[1]
    return block if roll == 0 else pltpu.roll(block, rows - roll, 1)


def rows_sum(block, weights):
    total = None
    for roll, weight in enumerate(weights):
        term = weight[None] * rolled_rows(block, roll)
        total = term if total is None else total + term
    return total


def kernel(nx, ny, nz, cuts, early, fields, strength_in, out, strength, u, acc, tiles, xs, ys, packed, landed, via,
           in_sem, sent, x_recv, y_send, y_recv, z_recv, via_recv, answers, turn):
    species, cx, cy, cz = u.shape
    groups = cz // SLOT
    rows_packed = packed.shape[1]
    px, py, pz = lax.axis_index("gx"), lax.axis_index("gy"), lax.axis_index("gz")
    x_left, x_right = lax.rem(px + nx - 1, nx), lax.rem(px + 1, nx)
    y_left, y_right = lax.rem(py + ny - 1, ny), lax.rem(py + 1, ny)
    z_left, z_right = lax.rem(pz + nz - 1, nz), lax.rem(pz + 1, nz)
    y_peers = [y_right] if ny == 2 else [y_right, y_left]

    barrier = pltpu.get_barrier_semaphore()
    to_left, to_right = (px, py, z_left), (px, py, z_right)
    left_x, right_x = (x_left, py, pz), (x_right, py, pz)
    first_z, last_z = pz == 0, pz == nz - 1

    def tell(semaphore, peer):
        pl.semaphore_signal(semaphore, inc=1, device_id=peer, device_id_type=MESH)

    for peer in y_peers:
        tell(barrier, (px, peer, pz))
    odd = lax.rem(px, 2) == 1
    paired = nx % 2 == 0

    def both_x(semaphore):
        tell(semaphore, left_x)
        tell(semaphore, right_x)

    if paired:
        pl.when(odd)(lambda: both_x(barrier))
    else:
        both_x(barrier)
    pl.when(pz < nz - 1)(lambda: tell(barrier, to_right))

    spans = []
    begin = 0
    for size in cuts:
        spans.append((begin, size))
        begin += size
    load = pltpu.make_async_copy(fields, u, in_sem)
    gains = pltpu.make_async_copy(strength_in, strength, in_sem)
    unloaded = lax.rem(py, 2) == 1
    pl.when(jnp.logical_not(unloaded))(load.start)

    held = early < len(cuts)
    mark = sum(cuts[:early])

    def y_row(k, source):
        part = pl.ds(*spans[k])
        return [
            pltpu.make_async_remote_copy(
                src_ref=source.at[part], dst_ref=ys.at[side, part],
                send_sem=y_send.at[side] if k < early else sent, recv_sem=y_recv.at[side, k],
                device_id=(px, peer, pz), device_id_type=MESH)
            for side, peer in enumerate(y_peers)]

    y_copies = [y_row(k, fields if k < early else u) for k in range(len(spans))]
    loaded_copies = [y_row(k, u) for k in range(early)]
    x_copies = [
        pltpu.make_async_remote_copy(
            src_ref=u.at[:, pl.ds(begin, REACH)], dst_ref=xs.at[side],
            send_sem=sent, recv_sem=x_recv,
            device_id=(peer, py, pz), device_id_type=MESH)
        for side, (begin, peer) in enumerate(((cx - REACH, x_right), (0, x_left)))
    ]

    relayed = held and ny == 2 and nz > 1 and nx > 2 and cx > 2 * via.shape[1]
    by_z, by_x = jnp.logical_and(px == 1, pz == 1), jnp.logical_and(px == 2, pz == 0)
    upper = py == 1
    source = jnp.logical_and(upper, jnp.logical_and(px == 1, pz == 0))
    relay = jnp.logical_or(by_z, by_x)
    relay_out = jnp.logical_and(upper, relay)
    back_z, back_x = jnp.logical_and(py == 0, by_z), jnp.logical_and(py == 0, by_x)
    turned, thick = pl.ds(*spans[early - 1]), via.shape[1]
    over_z, over_x, straight = pl.ds(0, thick), pl.ds(thick, thick), pl.ds(2 * thick, cx - 2 * thick)

    def hop(src, dst, send_sem, recv_sem, peer):
        return pltpu.make_async_remote_copy(
            src_ref=src, dst_ref=dst, send_sem=send_sem, recv_sem=recv_sem, device_id=peer, device_id_type=MESH)

    if relayed:
        across_y = (px, y_right, pz)
        direct = hop(fields.at[turned, straight], ys.at[0, turned, straight], y_send.at[0], y_recv.at[0, early - 1], across_y)
        out_z = hop(u.at[turned, over_z], via, y_send.at[0], via_recv, to_right)
        out_x = hop(u.at[turned, over_x], via, y_send.at[0], via_recv, right_x)
        over = hop(via, via, sent, via_recv, across_y)
        home_z = hop(via, ys.at[0, turned, over_z], sent, y_recv.at[0, early - 1], to_left)
        home_x = hop(via, ys.at[0, turned, over_x], sent, y_recv.at[0, early - 1], left_x)

    def settle(ref, semaphore):
        pltpu.make_async_copy(ref, ref, semaphore).wait()

    def start_y(rows):
        for row in rows:
            for copy in row:
                copy.start()

    def early_sent():
        for side in range(len(y_peers)):
            settle(u.at[pl.ds(0, mark)], y_send.at[side])

    greeters = (pz > 0).astype(jnp.int32) + (2 * (1 - lax.rem(px, 2)) if paired else 2)
    pl.semaphore_wait(barrier, len(y_peers) + greeters)
    def start_early():
        if relayed:
            start_y(y_copies[:early - 1])
            pl.when(source)(direct.start)
            pl.when(jnp.logical_not(source))(lambda: start_y(y_copies[early - 1:early]))
        else:
            start_y(y_copies[:early])

    pl.when(unloaded)(start_early)
    pl.when(unloaded)(load.start)
    load.wait()
    pl.when(jnp.logical_not(unloaded))(lambda: start_y(loaded_copies))
    gains.start()
    if held:
        at_once = jnp.logical_not(jnp.logical_or(odd, relay_out) if relayed else odd)
        pl.when(at_once)(lambda: start_y(y_copies[early:]))
    if paired:
        pl.when(jnp.logical_not(odd))(lambda: both_x(answers.at[0]))
    pl.when(pz > 0)(lambda: tell(answers.at[1], to_left))
    pl.when(last_z)(lambda: tell(answers.at[2], to_left))
    if paired:
        pl.when(odd)(lambda: pl.semaphore_wait(answers.at[0], 2))
    if relayed:
        pl.when(source)(out_x.start)
    for copy in x_copies:
        copy.start()

    lane = lax.broadcasted_iota(jnp.int32, (cx, cy, cz), 2)
    slot = lane // SLOT
    for p in range(rows_packed):
        first = p * groups
        here = min(groups, species - first)

        def pack(g, carry):
            head, tail = carry
            v = u[first + g]
            mine = slot == g
            head = jnp.where(mine, pltpu.roll(v, g * SLOT, 2), head)
            tail = jnp.where(mine, pltpu.roll(v, lax.rem((g + 1) * SLOT, cz), 2), tail)
            return head, tail

        zero = jnp.zeros((cx, cy, cz), jnp.float32)
        head, tail = each(0, here, AT_ONCE[0], pack, (zero, zero))
        packed[0, p] = head
        packed[1, p] = tail

    z_copies = [
        pltpu.make_async_remote_copy(
            src_ref=packed.at[side], dst_ref=landed.at[side],
            send_sem=sent, recv_sem=z_recv,
            device_id=(px, py, peer), device_id_type=MESH)
        for side, peer in enumerate((z_left, z_right))
    ]

    gains.wait()

    def start_right():
        pl.semaphore_wait(answers.at[1], 1)
        z_copies[1].start()

    def pass_token():
        pl.semaphore_wait(answers.at[2], 1)
        tell(answers.at[2], to_left)

    def close_ring():
        pl.semaphore_wait(answers.at[2], 1)
        tell(answers.at[1], to_left)
        z_copies[0].start()

    def end_ring():
        pl.semaphore_wait(answers.at[1], 1)
        z_copies[1].start()

    def forward(hop):
        settle(via, via_recv)
        hop.start()

    pl.when(pz < nz - 1)(start_right)
    if relayed:
        pl.when(source)(out_z.start)
    pl.when(pz > 0)(z_copies[0].start)
    pl.when(jnp.logical_and(pz > 0, pz < nz - 1))(pass_token)
    pl.when(first_z)(close_ring)

    own = [row_weights(cy, cz, r, (0,)) for r in range(cy)]
    if ny == 2:
        remote = [[row_weights(cy, cz, r, (cy, -cy)) for r in range(cy)]]
    else:
        remote = [[row_weights(cy, cz, r, (base,)) for r in range(cy)] for base in (-cy, cy)]
    inside = lane_weights(cz, (0,), 2.0 * WEIGHTS[0])
    across = lane_weights(cz, (cz, -cz), WEIGHTS[0])

    def along_own(s, _):
        v = u[s]
        total = along_lanes(v.reshape(cx * cy, cz), inside).reshape(cx, cy, cz)
        acc[s] = total + rows_sum(v, own)
        return 0

    each(0, species, AT_ONCE[1], along_own)
    pl.when(last_z)(end_ring)
    settle(landed, z_recv)

    def along_z(s, _):
        p, g = s // groups, lax.rem(s, groups)
        after = pltpu.roll(landed[0, p], lax.rem(cz - g * SLOT, cz), 2)
        before = pltpu.roll(landed[1, p], cz - (g + 1) * SLOT, 2)
        halo = jnp.where(lane < cz // 2, after, before)
        acc[s] = acc[s] + along_lanes(halo.reshape(cx * cy, cz), across).reshape(cx, cy, cz)
        return 0

    each(0, species, AT_ONCE[2], along_z)
    if relayed:
        def forward_out():
            forward(over)
            pl.when(jnp.logical_not(odd))(lambda: start_y(y_copies[early:]))

        pl.when(relay_out)(forward_out)

    def along_x(s, _):
        cells = [xs[0, s, i] for i in range(REACH)] + [u[s, i] for i in range(cx)]
        cells += [xs[1, s, i] for i in range(REACH)]
        for i in range(cx):
            total = acc[s, i]
            for d in range(1, REACH + 1):
                total = total + WEIGHTS[d] * (cells[REACH + i - d] + cells[REACH + i + d])
            acc[s, i] = total
        return 0

    def along_y(s, _):
        total = acc[s]
        for side, weights in enumerate(remote):
            total = total + rows_sum(ys[side, s], weights)
        out[s] = u[s] + (strength[s] * (1.0 / 1024.0)) * total
        return 0

    def go_on():
        pl.semaphore_wait(turn, 1)
        start_y(y_copies[early:])

    def pass_on():
        early_sent()
        tell(turn, right_x)

    if held:
        pl.when(jnp.logical_not(odd))(pass_on)
    if relayed:
        pl.when(back_x)(lambda: forward(home_x))
    settle(xs, x_recv)
    lax.fori_loop(0, species, along_x, 0)
    if held:
        pl.when(odd)(go_on)
    if relayed:
        pl.when(back_z)(lambda: forward(home_z))
    for k, (begin, size) in enumerate(spans):
        for side in range(len(y_peers)):
            settle(ys.at[side, pl.ds(begin, size)], y_recv.at[side, k])
        lax.fori_loop(begin, begin + size, along_y, 0)
    if held:
        pl.when(odd)(early_sent)
    else:
        early_sent()
    layers = 2 * species * REACH + 2 * rows_packed * cx + len(y_peers) * (species - mark) * cx
    if relayed:
        pl.when(relay)(lambda: settle(tiles.at[pl.ds(0, layers + via.shape[0] * thick)], sent))
        pl.when(jnp.logical_not(relay))(lambda: settle(tiles.at[pl.ds(0, layers)], sent))
    else:
        settle(tiles.at[pl.ds(0, layers)], sent)


def write(filtered, out, done):
    for s in range(filtered.shape[0]):
        pltpu.make_async_copy(filtered.at[s], out.at[s], done).start()
    pltpu.make_async_copy(filtered, out, done).wait()


def local(nx, ny, nz, fields, strength):
    species, cx, cy, cz = fields.shape
    cuts = CUTS if sum(CUTS) == species else (1,) * species
    pieces = len(cuts)
    early = EARLY if sum(CUTS) == species and nx % 2 == 0 else pieces
    sides = 1 if ny == 2 else 2
    groups = cz // SLOT
    rows_packed = -(-species // groups)
    block = (species, cx, cy, cz)
    layers = 2 * species * REACH + 2 * rows_packed * cx + sides * species * cx + species * DETOUR
    dma = pltpu.SemaphoreType.DMA
    filtered = pl.pallas_call(
        functools.partial(kernel, nx, ny, nz, cuts, early),
        out_shape=pltpu.VMEM(block, jnp.float32),
        in_specs=[pl.BlockSpec(memory_space=pltpu.HBM), pl.BlockSpec(memory_space=pl.ANY)],
        out_specs=pl.BlockSpec(memory_space=pltpu.VMEM),
        scratch_shapes=[
            pltpu.SMEM((species,), jnp.float32),
            pltpu.VMEM(block, jnp.float32),
            pltpu.VMEM(block, jnp.float32),
            pltpu.VMEM((layers, cy, cz), jnp.float32),
            pltpu.VMEM((2, species, REACH, cy, cz), jnp.float32),
            pltpu.VMEM((sides,) + block, jnp.float32),
            pltpu.VMEM((2, rows_packed, cx, cy, cz), jnp.float32),
            pltpu.VMEM((2, rows_packed, cx, cy, cz), jnp.float32),
            pltpu.VMEM((cuts[early - 1], DETOUR, cy, cz), jnp.float32),
            dma,
            dma,
            dma,
            dma((sides,)),
            dma((sides, pieces)),
            dma,
            dma,
            pltpu.SemaphoreType.REGULAR((3,)),
            pltpu.SemaphoreType.REGULAR,
        ],
        compiler_params=pltpu.CompilerParams(collective_id=0, has_side_effects=True, vmem_limit_bytes=56 * 1024 * 1024),
        name="filter_pass",
    )(fields, strength)
    return pl.pallas_call(
        write,
        out_shape=pltpu.HBM(block, jnp.float32),
        in_specs=[pl.BlockSpec(memory_space=pltpu.VMEM)],
        out_specs=pl.BlockSpec(memory_space=pltpu.HBM),
        scratch_shapes=[dma],
        compiler_params=pltpu.CompilerParams(vmem_limit_bytes=4 * 1024 * 1024),
        name="write",
    )(filtered)


def solution(mesh):
    sizes = mesh.shape
    return jax.shard_map(
        functools.partial(local, sizes["gx"], sizes["gy"], sizes["gz"]),
        mesh=mesh,
        in_specs=(P(None, "gx", "gy", "gz"), P()),
        out_specs=P(None, "gx", "gy", "gz"),
        check_vma=False,
    )
```
